512 devices in a mesh: line: 4 (over z_lo), tx: 8 (over z_hi, core), ty: 16 (over y, x).
Axes of the slice: x: 4, y: 4, z: 16 (z_hi: 4, z_lo: 4; z = z_hi * 4 + z_lo), core: 2. Of those that a mesh axis runs over, the one named last changes fastest.
Arguments:
- right_side: float32 [16, 32, 64, 128], P('line', 'tx', 'ty'), may hold values from -3 to 3
- start_field: float32 [16, 32, 64, 128], P('line', 'tx', 'ty'), may hold values from -3 to 3
- line_inverse: bfloat16 [16, 32, 64, 128, 128], P('line', 'tx', 'ty'), as said below
- lower_scale: float32 [16, 32, 64], P('line', 'tx', 'ty'), may hold values from 0.85 to 1
- upper_scale: float32 [16, 32, 64], P('line', 'tx', 'ty'), may hold values from 0.85 to 1
- lower_block: float32 [128, 128], replicated
- upper_block: float32 [128, 128], replicated
- face_blocks: float32 [4, 128, 128], replicated, may hold values from -0.15625 to 0.15625
- face_kind: int32 [4, 16, 32, 64], P(None, 'line', 'tx', 'ty'), may hold values from 0 to 3
- face_scale: float32 [4, 16, 32, 64], P(None, 'line', 'tx', 'ty'), may hold values from 0.25 to 1
- agglomerate: int32 [16, 32, 64], P('line', 'tx', 'ty'), may hold values from 0 to 255
- restriction: float32 [32, 128], replicated, may hold values from -0.5 to 0.5
- coarse_inverse: float32 [4, 8, 256, 32, 32], P('line', 'tx', 'ty'), as said below
Outputs:
- corrected: float32 [16, 32, 64, 128], P('line', 'tx', 'ty')
- residual: float32 [16, 32, 64, 128], P('line', 'tx', 'ty')
The draws below stay inside these ranges and needn't reach their ends.
Inputs may be any that keep to these rules, and one draw needn't show every extreme that they name: An element's agglomerate is one of the 256 agglomerates of its own column. `line_inverse`: each block is a diagonal of positive entries plus a full-rank part. `coarse_inverse`: each block is a diagonal of positive entries plus a full-rank part.
All inputs are finite; a program needn't handle non-finite values.
Results may differ from the reference program's by a relative error of at most 0.0003.
Values sent between devices are 32-bit elements; how exact they have to be, the bound alone decides.
No kernel may reach another device: no remote copies, remote signals or barrier semaphores. Data moves between devices by JAX's collectives and lax.ppermute only.
A program may use at most 64 MiB of HBM per device.

```python
import math
import jax
import jax.numpy as jnp
from jax import lax

B = 128
CB = 32
SWEEPS = 2
SEG = 4
LX = 4
LINES = 16
NX = 32
NY = 64
NAGG = 256
N_LINE = 4
N_TX = 8


def draw_line_inverse(key, part):
    slab_keys = jax.random.split(key, LINES)

    def one_slab(slab_key):
        diag_key, jitter_key = jax.random.split(slab_key)
        diagonal = jnp.exp(jax.random.uniform(diag_key, (NX, NY, B), jnp.float32, math.log(0.85), math.log(1.1)))
        jitter = 0.2 * jax.random.normal(jitter_key, (NX, NY, B, B), jnp.float32) * B ** (-0.5)
        return (jitter + diagonal[..., None] * jnp.eye(B, dtype=jnp.float32)).astype(jnp.bfloat16)
    return lax.map(one_slab, slab_keys)


def coupling_block(block_key):
    jitter = 0.2 * jax.random.normal(block_key, (B, B), jnp.float32) * B ** (-0.5)
    return jnp.eye(B, dtype=jnp.float32) + jitter


def draw_lower_block(key, part):
    return coupling_block(jax.random.fold_in(key, 11))


def draw_upper_block(key, part):
    return coupling_block(jax.random.fold_in(key, 23))


def draw_coarse_inverse(key, part):
    diag_key, jitter_key = jax.random.split(jax.random.fold_in(key, 37))
    diagonal = jnp.exp(jax.random.uniform(diag_key, (N_LINE, N_TX, NAGG, CB), jnp.float32, math.log(0.5), math.log(2.0)))
    jitter = 0.3 * jax.random.normal(jitter_key, (N_LINE, N_TX, NAGG, CB, CB), jnp.float32) * CB ** (-0.5)
    return jitter + diagonal[..., None] * jnp.eye(CB, dtype=jnp.float32)


def set_ends(drawn, rng, least, top_value):
    extent = drawn.shape
    index_at = [jax.random.randint(jax.random.fold_in(rng, axis), (), 0, extent[axis]) for axis in range(len(extent))]
    drawn = drawn.at[tuple(index_at)].set(least)
    longest = extent.index(max(extent))
    index_at[longest] = (index_at[longest] + 1) % extent[longest]
    return drawn.at[tuple(index_at)].set(top_value)


def level_of(own_key, dims, pieces, low, largest):
    def one(position, parts):
        draws = jax.random.uniform(jax.random.fold_in(jax.random.fold_in(own_key, 6), position), (parts,), jnp.float32, low / len(pieces), largest / len(pieces))
        return jnp.repeat(jnp.exp(draws), dims[position] // parts).reshape((-1,) + (1,) * (len(dims) - position - 1))

    level = one(*pieces[0])
    for cut in pieces[1:]:
        level = level * one(*cut)
    return level


def noise(key, dims, scale, limit, shards=(), kind=jnp.bfloat16):
    entries = jax.random.normal(key, dims, jnp.float32) * scale
    if len(shards) > 0:
        entries = level_of(key, dims, shards, -0.22, 0.18) * entries
    return jnp.clip(entries, min=-limit, max=limit).astype(kind)


def setup_inputs(seed: int = 0) -> dict:
    key_list = jax.random.split(jax.random.key(seed), 14)
    right_side = noise(key_list[0], (LINES, NX, NY, B), 0.5, 3.0, ((0, 4), (1, 8), (2, 16)), jnp.float32)
    start_field = noise(key_list[1], (LINES, NX, NY, B), 0.5, 3.0, ((0, 4), (1, 8), (2, 16)), jnp.float32)
    line_inverse = draw_line_inverse(jax.random.fold_in(key_list[13], 71), 0)
    lower_scale = jnp.clip(jnp.exp(math.log(1.0) - 0.1625189 * jax.random.uniform(key_list[3], (LINES, NX, NY), jnp.float32) ** level_of(key_list[3], (LINES, NX, NY), ((0, 4), (1, 8), (2, 16)), -0.2, 0.2)), 0.85, 1.0)
    upper_scale = jnp.clip(jnp.exp(math.log(1.0) - 0.1625189 * jax.random.uniform(key_list[4], (LINES, NX, NY), jnp.float32) ** level_of(key_list[4], (LINES, NX, NY), ((0, 4), (1, 8), (2, 16)), -0.2, 0.2)), 0.85, 1.0)
    lower_block = draw_lower_block(jax.random.fold_in(key_list[13], 71), 0)
    upper_block = draw_upper_block(jax.random.fold_in(key_list[13], 71), 0)
    face_blocks = noise(key_list[7], (4, B, B), (11 * B) ** -0.5, 0.15625, (), jnp.float32)
    face_kind = set_ends(jax.random.randint(key_list[8], (4, LINES, NX, NY), 0, 4), jax.random.fold_in(key_list[8], 1), 0, 3).astype(jnp.int32)
    face_scale = jnp.clip(jnp.exp(math.log(1.0) - 1.3862944 * jax.random.uniform(key_list[9], (4, LINES, NX, NY), jnp.float32) ** level_of(key_list[9], (4, LINES, NX, NY), ((1, 4), (2, 8), (3, 16)), -0.2, 0.2)), 0.25, 1.0)
    agglomerate = set_ends(jax.random.randint(key_list[10], (LINES, NX, NY), 0, NAGG), jax.random.fold_in(key_list[10], 1), 0, NAGG - 1).astype(jnp.int32)
    restriction = noise(key_list[11], (CB, B), B ** -0.5, 0.5, (), jnp.float32)
    coarse_inverse = draw_coarse_inverse(jax.random.fold_in(key_list[13], 71), 0)
    return {"right_side": right_side, "start_field": start_field, "line_inverse": line_inverse, "lower_scale": lower_scale, "upper_scale": upper_scale, "lower_block": lower_block, "upper_block": upper_block, "face_blocks": face_blocks, "face_kind": face_kind, "face_scale": face_scale, "agglomerate": agglomerate, "restriction": restriction, "coarse_inverse": coarse_inverse}


highest = lax.Precision.HIGHEST


def couple(field, face_blocks, face_kind, face_scale):
    padded = jnp.pad(field, ((0, 0), (1, 1), (1, 1), (0, 0)))
    beside = (padded[:, :-2, 1:-1], padded[:, 2:, 1:-1], padded[:, 1:-1, :-2], padded[:, 1:-1, 2:])
    total = jnp.zeros_like(field)
    kinds = jnp.arange(4, dtype=jnp.int32)
    for side in range(4):
        images = jnp.einsum('sxyb,kcb->ksxyc', beside[side], face_blocks, precision=highest)
        chosen = (face_kind[side][None] == kinds[:, None, None, None]).astype(jnp.float32)
        picked = jnp.sum(chosen[..., None] * images, axis=0)
        total = total + face_scale[side][..., None] * picked
    return total


def forward(line_inverse, lower_scale, lower_block, drive, start):
    def step(carry, items):
        inverse, scale, source = items
        inner = source - scale[..., None] * jnp.einsum('cb,xyb->xyc', lower_block, carry, precision=highest)
        value = jnp.einsum('xycb,xyb->xyc', inverse.astype(jnp.float32), inner, precision=highest)
        return value, value
    final, values = lax.scan(step, start, (line_inverse, lower_scale, drive))
    return values


def backward(line_inverse, upper_scale, upper_block, ahead, start):
    def step(carry, items):
        inverse, scale, source = items
        inner = scale[..., None] * jnp.einsum('cb,xyb->xyc', upper_block, carry, precision=highest)
        value = source - jnp.einsum('xycb,xyb->xyc', inverse.astype(jnp.float32), inner, precision=highest)
        return value, value
    final, values = lax.scan(step, start, (line_inverse, upper_scale, ahead), reverse=True)
    return values


def reference(right_side, start_field, line_inverse, lower_scale, upper_scale, lower_block, upper_block, face_blocks, face_kind, face_scale, agglomerate, restriction, coarse_inverse):
    empty = jnp.zeros(right_side.shape[1:], jnp.float32)
    field = start_field
    previous = start_field
    for sweep in range(SWEEPS):
        previous = field
        drive = right_side - couple(previous, face_blocks, face_kind, face_scale)
        ahead = forward(line_inverse, lower_scale, lower_block, drive, empty)
        field = backward(line_inverse, upper_scale, upper_block, ahead, empty)
    residual = couple(previous - field, face_blocks, face_kind, face_scale)
    blocks = residual.reshape(N_LINE, SEG, N_TX, LX, NY, B).transpose(0, 2, 1, 3, 4, 5).reshape(N_LINE, N_TX, SEG * LX * NY, B)
    owners = agglomerate.reshape(N_LINE, SEG, N_TX, LX, NY).transpose(0, 2, 1, 3, 4).reshape(N_LINE, N_TX, SEG * LX * NY)
    chosen = (owners[..., None] == jnp.arange(NAGG, dtype=jnp.int32)).astype(jnp.float32)
    projected = jnp.einsum('cb,lteb->ltec', restriction, blocks, precision=highest)
    coarse_sums = jnp.einsum('ltea,ltec->ltac', chosen, projected, precision=highest)
    update = jnp.einsum('ltacd,ltad->ltac', coarse_inverse, coarse_sums, precision=highest)
    spread = jnp.einsum('ltea,ltac->ltec', chosen, update, precision=highest)
    fine = jnp.einsum('cb,ltec->lteb', restriction, spread, precision=highest)
    correction = fine.reshape(N_LINE, N_TX, SEG, LX, NY, B).transpose(0, 2, 1, 3, 4, 5).reshape(right_side.shape)
    return field + correction, residual
```

```python
import functools

import jax
import jax.numpy as jnp
from jax import lax
from jax.experimental import pallas as pl
from jax.experimental.pallas import tpu as pltpu
from jax.sharding import PartitionSpec as P

SWEEPS = 2
F32 = jnp.float32
BF16 = jnp.bfloat16
SPEC = pl.BlockSpec(memory_space=pltpu.VMEM)


def call(kernel, outs, *args, scratch=()):
    return pl.pallas_call(
        kernel,
        in_specs=[SPEC] * len(args),
        out_specs=[SPEC] * len(outs),
        out_shape=[pltpu.VMEM(s, d) for s, d in outs],
        scratch_shapes=list(scratch),
    )(*[pltpu.with_memory_space_constraint(a, pltpu.VMEM) for a in args])


def halves(v):
    hi = v.astype(BF16)
    return hi, (v - hi.astype(F32)).astype(BF16)


def nt(a, b):
    return lax.dot_general(a, b, (((1,), (1,)), ((), ())), preferred_element_type=F32)


def nn(a, b):
    return lax.dot_general(a, b, (((1,), (0,)), ((), ())), preferred_element_type=F32)


def times(v, m, dot=nt):
    n = v.shape[0]
    hi, lo = halves(v)
    both = dot(jnp.concatenate([hi, lo], 0), m[0])
    return both[:n] + both[n:] + dot(hi, m[1])


def each_line(v, weights, lines):
    hi, lo = halves(v)
    out = nt(jnp.concatenate([hi, lo], 0), weights)
    row = lax.broadcasted_iota(jnp.int32, (2 * lines, 128), 0)
    row = jnp.where(row >= lines, row - lines, row)
    acc = jnp.zeros((2 * lines, 128), F32)
    for l in range(lines):
        acc = acc + jnp.where(row == l, out[:, l * 128 : (l + 1) * 128], 0.0)
    return acc[:lines] + acc[lines:]


def forward(g, inc, w_ref, low, cols, n, lines):
    carry, ys = inc, []
    for i in range(n):
        at = slice(i * lines, (i + 1) * lines)
        inner = g[at] - cols[at, 16:17] * times(carry, low)
        carry = each_line(inner, w_ref[i * lines * 128 : (i + 1) * lines * 128, :], lines)
        ys.append(carry)
    return ys


def backward(y, arr, w_ref, upp, cols, n, lines):
    carry, xs = arr, [None] * n
    for i in reversed(range(n)):
        at = slice(i * lines, (i + 1) * lines)
        inner = cols[at, 17:18] * times(carry, upp)
        carry = y[at] - each_line(inner, w_ref[i * lines * 128 : (i + 1) * lines * 128, :], lines)
        xs[i] = carry
    return xs


def put_edges(x_ref, par_ref, outs, n, lx, ly):
    a_ref, b_ref, c_ref, d_ref = outs
    lines = lx * ly
    first = jnp.concatenate([x_ref[i * lines : i * lines + ly, :] for i in range(n)], 0)
    last = jnp.concatenate([x_ref[(i + 1) * lines - ly : (i + 1) * lines, :] for i in range(n)], 0)
    even = par_ref[0:1, :] < 0.5
    a_ref[...] = jnp.where(even, last, first)
    b_ref[...] = jnp.where(even, first, last)
    first = x_ref[pl.ds(0, n * lx, stride=ly), :]
    last = x_ref[pl.ds(ly - 1, n * lx, stride=ly), :]
    even = par_ref[1:2, :] < 0.5
    c_ref[...] = jnp.where(even, last, first)
    d_ref[...] = jnp.where(even, first, last)


def tangential(x_ref, got, par_ref, cols, blocks, near, n, lx, ly):
    lines = lx * ly
    x = x_ref[...]
    even = par_ref[0:1, :] < 0.5
    a, b, c, d = (r[...] for r in got)
    below, above = jnp.where(even, b, a), jnp.where(even, a, b)
    near[0] = pltpu.roll(x, ly, 0)
    near[1] = pltpu.roll(x, n * lines - ly, 0)
    for i in range(n):
        near[0, i * lines : i * lines + ly, :] = below[i * ly : (i + 1) * ly]
        near[1, (i + 1) * lines - ly : (i + 1) * lines, :] = above[i * ly : (i + 1) * ly]
    even = par_ref[1:2, :] < 0.5
    below, above = jnp.where(even, d, c), jnp.where(even, c, d)
    row = lax.broadcasted_iota(jnp.int32, x.shape, 0) % ly
    near[2] = pltpu.roll(x, 1, 0)
    near[3] = pltpu.roll(x, n * lines - 1, 0)
    for q in range(n * lx):
        near[2, q * ly : q * ly + 1, :] = below[q : q + 1]
        near[3, q * ly + ly - 1 : q * ly + ly, :] = above[q : q + 1]
    total = jnp.zeros(x.shape, F32)
    beside = [near[s] for s in range(4)]
    for k in range(4):
        mixed = sum(cols[:, 4 * s + k : 4 * s + k + 1] * beside[s] for s in range(4))
        total = total + times(mixed, (blocks[0][k], blocks[1][k]))
    return total


def swaps(count, start):
    return [
        pair
        for i in range(start, count - 1, 2)
        for pair in ((i, i + 1), (i + 1, i))
    ]


def exchange(sends):
    nx, ny = lax.axis_size("tx"), lax.axis_size("ty")
    a, b, c, d = sends
    return (
        lax.ppermute(a, "tx", swaps(nx, 0)),
        lax.ppermute(b, "tx", swaps(nx, 1)),
        lax.ppermute(c, "ty", swaps(ny, 0)),
        lax.ppermute(d, "ty", swaps(ny, 1)),
    )


def body(
    right_side,
    start_field,
    line_inverse,
    lower_scale,
    upper_scale,
    lower_block,
    upper_block,
    face_blocks,
    face_kind,
    face_scale,
    agglomerate,
    restriction,
    coarse_inverse,
):
    n, lx, ly, width = right_side.shape
    lines, rows, cb = lx * ly, n * lx * ly, restriction.shape[0]
    quarter = width // cb
    segments, owners = lax.axis_size("line"), lax.axis_size("ty")
    owned_rows = coarse_inverse.shape[2] // quarter
    agg_rows = owned_rows * owners
    rhs = right_side.reshape(rows, width)
    start = start_field.reshape(rows, width)
    w = line_inverse.reshape(rows * width, width)

    kinds = jnp.arange(4, dtype=jnp.int32)
    face = jnp.where(face_kind[:, None] == kinds[None, :, None, None, None], face_scale[:, None], 0.0)
    agg = agglomerate.reshape(rows)
    agg_row, agg_part = agg // quarter, agg % quarter
    cols = jnp.concatenate(
        [
            face.reshape(16, rows),
            lower_scale.reshape(1, rows),
            upper_scale.reshape(1, rows),
            agg_row.astype(F32)[None],
            agg_part.astype(F32)[None],
            jnp.zeros((12, rows), F32),
        ],
        0,
    ).T
    agg_lane = jnp.broadcast_to(agg_row.astype(F32)[None], (8, rows))
    par = jnp.stack([lax.axis_index("tx") % 2, lax.axis_index("ty") % 2]).astype(F32)
    par = jnp.broadcast_to(jnp.pad(par, (0, 6))[:, None], (8, width))
    eye = jnp.eye(quarter, dtype=F32)
    ci = coarse_inverse.reshape(owned_rows, quarter, cb, 1, cb) * eye[None, :, None, :, None]
    ci = ci.reshape(owned_rows * width, width)
    spread_op = jnp.tile(restriction, (quarter, 1))

    block, edge = ((rows, width), F32), ((lines, width), F32)
    half, half4 = ((width, width), BF16), ((4, width, width), BF16)
    edges4 = [((n * ly, width), F32)] * 2 + [((n * lx, width), F32)] * 2

    def prepare(x_ref, par_ref, l_ref, u_ref, f_ref, r_ref, c_ref, *outs):
        put_edges(x_ref, par_ref, outs[:4], n, lx, ly)
        for src, k in ((l_ref, 4), (u_ref, 6), (f_ref, 8), (r_ref, 10), (c_ref, 12)):
            outs[k][...], outs[k + 1][...] = halves(src[...])

    made = call(
        prepare,
        edges4
        + [half, half, half, half, half4, half4, half, half]
        + [((owned_rows * width, width), BF16)] * 2,
        start,
        par,
        lower_block,
        upper_block,
        face_blocks,
        spread_op,
        ci,
    )
    sends, lh, ll, uh, ul, fh, fl, rh, rl, ch, cl = made[:4], *made[4:]

    def open_forward(x_ref, a, b, c, d, par_ref, cols_ref, fh_ref, fl_ref, rhs_ref, lh_ref, ll_ref, w_ref, g_ref, y_ref, f_ref, near):
        cols = cols_ref[...]
        total = tangential(x_ref, (a, b, c, d), par_ref, cols, (fh_ref, fl_ref), near, n, lx, ly)
        g = rhs_ref[...] - total
        g_ref[...] = g
        zero = jnp.zeros((lines, width), F32)
        ys = forward(g, zero, w_ref, (lh_ref[...], ll_ref[...]), cols, n, lines)
        y_ref[...] = jnp.concatenate(ys, 0)
        f_ref[...] = ys[-1]

    def next_forward(g_ref, inc_ref, got_ref, cols_ref, lh_ref, ll_ref, w_ref, sum_ref, f_ref):
        inc = inc_ref[...] + got_ref[...]
        sum_ref[...] = inc
        ys = forward(g_ref[...], inc, w_ref, (lh_ref[...], ll_ref[...]), cols_ref[...], n, lines)
        f_ref[...] = ys[-1]

    def turn(g_ref, inc_ref, got_ref, cols_ref, lh_ref, ll_ref, uh_ref, ul_ref, w_ref, y_ref, x_ref):
        cols = cols_ref[...]
        inc = inc_ref[...] + got_ref[...]
        ys = forward(g_ref[...], inc, w_ref, (lh_ref[...], ll_ref[...]), cols, n, lines)
        y = jnp.concatenate(ys, 0)
        y_ref[...] = y
        zero = jnp.zeros((lines, width), F32)
        xs = backward(y, zero, w_ref, (uh_ref[...], ul_ref[...]), cols, n, lines)
        x_ref[...] = xs[0]

    def next_backward(y_ref, arr_ref, got_ref, cols_ref, uh_ref, ul_ref, w_ref, sum_ref, x_ref):
        arr = arr_ref[...] + got_ref[...]
        sum_ref[...] = arr
        xs = backward(y_ref[...], arr, w_ref, (uh_ref[...], ul_ref[...]), cols_ref[...], n, lines)
        x_ref[...] = xs[0]

    def close_backward(last, y_ref, arr_ref, got_ref, prev_ref, par_ref, cols_ref, uh_ref, ul_ref, w_ref, x_ref, d_ref, *outs):
        arr = arr_ref[...] + got_ref[...]
        xs = backward(y_ref[...], arr, w_ref, (uh_ref[...], ul_ref[...]), cols_ref[...], n, lines)
        x = jnp.concatenate(xs, 0)
        x_ref[...] = x
        d_ref[...] = prev_ref[...] - x
        put_edges(d_ref if last else x_ref, par_ref, outs, n, lx, ly)

    field = start
    change = None
    for sweep in range(SWEEPS):
        got = exchange(sends)
        g, y, ahead = call(
            open_forward,
            [block, block, edge],
            field, *got, par, cols, fh, fl, rhs, lh, ll, w,
            scratch=[pltpu.VMEM((4, rows, width), F32)],
        )
        inc = jnp.zeros((lines, width), F32)
        for k in range(segments - 2):
            recv = lax.ppermute(ahead, "line", [(k, k + 1)])
            inc, ahead = call(next_forward, [edge, edge], g, inc, recv, cols, lh, ll, w)
        recv = lax.ppermute(ahead, "line", [(segments - 2, segments - 1)])
        y, behind = call(turn, [block, edge], g, inc, recv, cols, lh, ll, uh, ul, w)
        arr = jnp.zeros((lines, width), F32)
        for k in range(segments - 2):
            recv = lax.ppermute(behind, "line", [(segments - 1 - k, segments - 2 - k)])
            arr, behind = call(next_backward, [edge, edge], y, arr, recv, cols, uh, ul, w)
        recv = lax.ppermute(behind, "line", [(1, 0)])
        out = call(
            functools.partial(close_backward, sweep == SWEEPS - 1),
            [block, block] + edges4,
            y, arr, recv, field, par, cols, uh, ul, w,
        )
        field, change, sends = out[0], out[1], out[2:]

    got = exchange(sends)

    def restrict(x_ref, a, b, c, d, par_ref, cols_ref, fh_ref, fl_ref, rh_ref, rl_ref, lane_ref, res_ref, part_ref, near):
        cols = cols_ref[...]
        res = tangential(x_ref, (a, b, c, d), par_ref, cols, (fh_ref, fl_ref), near, n, lx, ly)
        res_ref[...] = res
        proj = times(res, (rh_ref[...], rl_ref[...]))
        part = lax.broadcasted_iota(jnp.int32, (rows, width), 1) // cb
        proj = jnp.where(part.astype(F32) == cols[:, 19:20], proj, 0.0)
        hit = lax.broadcasted_iota(jnp.int32, (agg_rows, rows), 0).astype(F32)
        hit = jnp.where(hit == lane_ref[0:1, :], 1.0, 0.0).astype(BF16)
        hi, lo = halves(proj)
        part_ref[...] = nn(hit, hi) + nn(hit, lo)

    residual, partial = call(
        restrict,
        [block, ((agg_rows, width), F32)],
        change, *got, par, cols, fh, fl, rh, rl, agg_lane,
        scratch=[pltpu.VMEM((4, rows, width), F32)],
    )
    parts = lax.all_to_all(partial.reshape(owners, owned_rows, width), "ty", 0, 0, tiled=True)

    def solve_coarse(parts_ref, ch_ref, cl_ref, up_ref):
        sums = parts_ref[0]
        for k in range(1, owners):
            sums = sums + parts_ref[k]
        hi, lo = halves(sums)
        zero = jnp.zeros((8 - owned_rows, width), BF16)
        hi, lo = jnp.concatenate([hi, zero], 0), jnp.concatenate([lo, zero], 0)
        both = jnp.concatenate([hi, lo], 0)
        out = nt(both, ch_ref[...])
        out = out[:8] + out[8:] + nt(both, cl_ref[...])[:8]
        row = lax.broadcasted_iota(jnp.int32, (8, width), 0)
        acc = jnp.zeros((8, width), F32)
        for k in range(owned_rows):
            acc = acc + jnp.where(row == k, out[:, k * width : (k + 1) * width], 0.0)
        for k in range(owners):
            up_ref[k] = acc[:owned_rows]

    (copies,) = call(solve_coarse, [((owners, owned_rows, width), F32)], parts, ch, cl)
    update = lax.all_to_all(copies, "ty", 0, 0, tiled=True)

    def correct(up_ref, x_ref, cols_ref, rh_ref, rl_ref, out_ref):
        cols = cols_ref[...]
        hit = lax.broadcasted_iota(jnp.int32, (rows, agg_rows), 1).astype(F32)
        hit = jnp.where(hit == cols[:, 18:19], 1.0, 0.0).astype(BF16)
        hi, lo = halves(up_ref[...])
        picked = nn(hit, hi) + nn(hit, lo)
        part = lax.broadcasted_iota(jnp.int32, (rows, width), 1) // cb
        picked = jnp.where(part.astype(F32) == cols[:, 19:20], picked, 0.0)
        out_ref[...] = x_ref[...] + times(picked, (rh_ref[...], rl_ref[...]), nn)

    (corrected,) = call(correct, [block], update.reshape(agg_rows, width), field, cols, rh, rl)
    return corrected.reshape(right_side.shape), residual.reshape(right_side.shape)


def solution(mesh):
    in_specs = (
        P("line", "tx", "ty", None),
        P("line", "tx", "ty", None),
        P("line", "tx", "ty", None, None),
        P("line", "tx", "ty"),
        P("line", "tx", "ty"),
        P(),
        P(),
        P(),
        P(None, "line", "tx", "ty"),
        P(None, "line", "tx", "ty"),
        P("line", "tx", "ty"),
        P(),
        P("line", "tx", "ty", None, None),
    )
    out_specs = (P("line", "tx", "ty", None), P("line", "tx", "ty", None))
    return jax.shard_map(body, mesh=mesh, in_specs=in_specs, out_specs=out_specs, check_vma=False)
```

```python
import functools

import jax
import jax.numpy as jnp
from jax import lax
from jax.experimental import pallas as pl
from jax.experimental.pallas import tpu as pltpu
from jax.sharding import PartitionSpec as P

SWEEPS = 2
F32 = jnp.float32
BF16 = jnp.bfloat16
SPEC = pl.BlockSpec(memory_space=pltpu.VMEM)


def call(kernel, outs, *args, scratch=(), whole=0):
    return pl.pallas_call(
        kernel,
        in_specs=[pl.BlockSpec(memory_space=pl.ANY)] * whole + [SPEC] * (len(args) - whole),
        out_specs=[SPEC] * len(outs),
        out_shape=[pltpu.VMEM(s, d) for s, d in outs],
        scratch_shapes=list(scratch),
        compiler_params=pltpu.CompilerParams(vmem_limit_bytes=24 << 20),
    )(*args[:whole], *[pltpu.with_memory_space_constraint(a, pltpu.VMEM) for a in args[whole:]])


def halves(v):
    hi = v.astype(BF16)
    return hi, (v - hi.astype(F32)).astype(BF16)


def nt(a, b):
    return lax.dot_general(a, b, (((1,), (1,)), ((), ())), preferred_element_type=F32)


def nn(a, b):
    return lax.dot_general(a, b, (((1,), (0,)), ((), ())), preferred_element_type=F32)


def times(v, m, dot=nt):
    n = v.shape[0]
    hi, lo = halves(v)
    both = dot(jnp.concatenate([hi, lo], 0), m[0])
    return both[:n] + both[n:] + dot(hi, m[1])


def each_line(v, weights, lines):
    hi, lo = halves(v)
    out = nt(jnp.concatenate([hi, lo], 0), weights)
    row = lax.broadcasted_iota(jnp.int32, (2 * lines, 128), 0)
    row = jnp.where(row >= lines, row - lines, row)
    acc = jnp.zeros((2 * lines, 128), F32)
    for l in range(lines):
        acc = acc + jnp.where(row == l, out[:, l * 128 : (l + 1) * 128], 0.0)
    return acc[:lines] + acc[lines:]


def forward(g, inc, w_ref, low, cols, n, lines):
    carry, ys = inc, []
    for i in range(n):
        at = slice(i * lines, (i + 1) * lines)
        inner = g[at] - cols[at, 16:17] * times(carry, low)
        carry = each_line(inner, w_ref[i * lines * 128 : (i + 1) * lines * 128, :], lines)
        ys.append(carry)
    return ys


def backward(y, arr, w_ref, upp, cols, n, lines):
    carry, xs = arr, [None] * n
    for i in reversed(range(n)):
        at = slice(i * lines, (i + 1) * lines)
        inner = cols[at, 17:18] * times(carry, upp)
        carry = y[at] - each_line(inner, w_ref[i * lines * 128 : (i + 1) * lines * 128, :], lines)
        xs[i] = carry
    return xs


def put_edges(x_ref, par_ref, outs, n, lx, ly):
    a_ref, b_ref, c_ref, d_ref = outs
    lines = lx * ly
    first = jnp.concatenate([x_ref[i * lines : i * lines + ly, :] for i in range(n)], 0)
    last = jnp.concatenate([x_ref[(i + 1) * lines - ly : (i + 1) * lines, :] for i in range(n)], 0)
    even = par_ref[0:1, :] < 0.5
    a_ref[...] = jnp.where(even, last, first)
    b_ref[...] = jnp.where(even, first, last)
    first = x_ref[pl.ds(0, n * lx, stride=ly), :]
    last = x_ref[pl.ds(ly - 1, n * lx, stride=ly), :]
    even = par_ref[1:2, :] < 0.5
    c_ref[...] = jnp.where(even, last, first)
    d_ref[...] = jnp.where(even, first, last)


def tangential(x_ref, got, par_ref, cols, blocks, near, n, lx, ly):
    lines = lx * ly
    x = x_ref[...]
    even = par_ref[0:1, :] < 0.5
    b, c, d, a = (r[...] for r in got)
    below, above = jnp.where(even, b, a), jnp.where(even, a, b)
    near[0] = pltpu.roll(x, ly, 0)
    near[1] = pltpu.roll(x, n * lines - ly, 0)
    for i in range(n):
        near[0, i * lines : i * lines + ly, :] = below[i * ly : (i + 1) * ly]
        near[1, (i + 1) * lines - ly : (i + 1) * lines, :] = above[i * ly : (i + 1) * ly]
    even = par_ref[1:2, :] < 0.5
    below, above = jnp.where(even, d, c), jnp.where(even, c, d)
    row = lax.broadcasted_iota(jnp.int32, x.shape, 0) % ly
    near[2] = pltpu.roll(x, 1, 0)
    near[3] = pltpu.roll(x, n * lines - 1, 0)
    for q in range(n * lx):
        near[2, q * ly : q * ly + 1, :] = below[q : q + 1]
        near[3, q * ly + ly - 1 : q * ly + ly, :] = above[q : q + 1]
    total = jnp.zeros(x.shape, F32)
    beside = [near[s] for s in range(4)]
    for k in range(4):
        mixed = sum(cols[:, 4 * s + k : 4 * s + k + 1] * beside[s] for s in range(4))
        total = total + times(mixed, (blocks[0][k], blocks[1][k]))
    return total


def swaps(count, start):
    return [
        pair
        for i in range(start, count - 1, 2)
        for pair in ((i, i + 1), (i + 1, i))
    ]


def exchange(sends):
    nx, ny = lax.axis_size("tx"), lax.axis_size("ty")
    a, b, c, d = sends
    b = lax.ppermute(b, "tx", swaps(nx, 1))
    c = lax.ppermute(c, "ty", swaps(ny, 0))
    d = lax.ppermute(d, "ty", swaps(ny, 1))
    a = lax.ppermute(a, "tx", swaps(nx, 0))
    return b, c, d, a


def body(
    right_side,
    start_field,
    line_inverse,
    lower_scale,
    upper_scale,
    lower_block,
    upper_block,
    face_blocks,
    face_kind,
    face_scale,
    agglomerate,
    restriction,
    coarse_inverse,
):
    n, lx, ly, width = right_side.shape
    lines, rows, cb = lx * ly, n * lx * ly, restriction.shape[0]
    quarter = width // cb
    segments, owners = lax.axis_size("line"), lax.axis_size("ty")
    owned_rows = coarse_inverse.shape[2] // quarter
    agg_rows = owned_rows * owners
    rhs = right_side.reshape(rows, width)
    start = start_field.reshape(rows, width)
    w = line_inverse.reshape(rows * width, width)

    kinds = jnp.arange(4, dtype=jnp.int32)
    face = jnp.where(face_kind[:, None] == kinds[None, :, None, None, None], face_scale[:, None], 0.0)
    agg = agglomerate.reshape(rows)
    agg_row, agg_part = agg // quarter, agg % quarter
    cols = jnp.concatenate(
        [
            face.reshape(16, rows),
            lower_scale.reshape(1, rows),
            upper_scale.reshape(1, rows),
            agg_row.astype(F32)[None],
            agg_part.astype(F32)[None],
            jnp.zeros((12, rows), F32),
        ],
        0,
    ).T
    agg_lane = jnp.broadcast_to(agg_row.astype(F32)[None], (8, rows))
    par = jnp.stack([lax.axis_index("tx") % 2, lax.axis_index("ty") % 2]).astype(F32)
    par = jnp.broadcast_to(jnp.pad(par, (0, 6))[:, None], (8, width))
    eye = jnp.eye(quarter, dtype=F32)
    ci = coarse_inverse.reshape(owned_rows, quarter, cb, 1, cb) * eye[None, :, None, :, None]
    ci = ci.reshape(owned_rows * width, width)
    spread_op = jnp.tile(restriction, (quarter, 1))

    block, edge = ((rows, width), F32), ((lines, width), F32)
    half, half4 = ((width, width), BF16), ((4, width, width), BF16)
    edges4 = [((n * ly, width), F32)] * 2 + [((n * lx, width), F32)] * 2

    def first_edges(x_ref, par_ref, *outs):
        put_edges(x_ref, par_ref, outs, n, lx, ly)

    sends = call(first_edges, edges4, start, par)

    def prepare(w_ref, l_ref, u_ref, f_ref, r_ref, c_ref, *outs):
        copy = pltpu.make_async_copy(w_ref, outs[10], outs[11])
        copy.start()
        for k, src in enumerate((l_ref, u_ref, f_ref, r_ref, c_ref)):
            outs[2 * k][...], outs[2 * k + 1][...] = halves(src[...])
        copy.wait()

    lh, ll, uh, ul, fh, fl, rh, rl, ch, cl, w = call(
        prepare,
        [half, half, half, half, half4, half4, half, half]
        + [((owned_rows * width, width), BF16)] * 2
        + [((rows * width, width), BF16)],
        w,
        lower_block,
        upper_block,
        face_blocks,
        spread_op,
        ci,
        scratch=[pltpu.SemaphoreType.DMA],
        whole=1,
    )

    def open_forward(x_ref, a, b, c, d, par_ref, cols_ref, fh_ref, fl_ref, rhs_ref, lh_ref, ll_ref, w_ref, g_ref, y_ref, f_ref, near):
        cols = cols_ref[...]
        total = tangential(x_ref, (a, b, c, d), par_ref, cols, (fh_ref, fl_ref), near, n, lx, ly)
        g = rhs_ref[...] - total
        g_ref[...] = g
        zero = jnp.zeros((lines, width), F32)
        ys = forward(g, zero, w_ref, (lh_ref[...], ll_ref[...]), cols, n, lines)
        y_ref[...] = jnp.concatenate(ys, 0)
        f_ref[...] = ys[-1]

    def next_forward(g_ref, inc_ref, got_ref, cols_ref, lh_ref, ll_ref, w_ref, sum_ref, f_ref):
        inc = inc_ref[...] + got_ref[...]
        sum_ref[...] = inc
        ys = forward(g_ref[...], inc, w_ref, (lh_ref[...], ll_ref[...]), cols_ref[...], n, lines)
        f_ref[...] = ys[-1]

    def turn(g_ref, inc_ref, got_ref, cols_ref, lh_ref, ll_ref, uh_ref, ul_ref, w_ref, y_ref, x_ref):
        cols = cols_ref[...]
        inc = inc_ref[...] + got_ref[...]
        ys = forward(g_ref[...], inc, w_ref, (lh_ref[...], ll_ref[...]), cols, n, lines)
        y = jnp.concatenate(ys, 0)
        y_ref[...] = y
        zero = jnp.zeros((lines, width), F32)
        xs = backward(y, zero, w_ref, (uh_ref[...], ul_ref[...]), cols, n, lines)
        x_ref[...] = xs[0]

    def next_backward(y_ref, arr_ref, got_ref, cols_ref, uh_ref, ul_ref, w_ref, sum_ref, x_ref):
        arr = arr_ref[...] + got_ref[...]
        sum_ref[...] = arr
        xs = backward(y_ref[...], arr, w_ref, (uh_ref[...], ul_ref[...]), cols_ref[...], n, lines)
        x_ref[...] = xs[0]

    def close_backward(last, y_ref, arr_ref, got_ref, prev_ref, par_ref, cols_ref, uh_ref, ul_ref, w_ref, x_ref, d_ref, *outs):
        arr = arr_ref[...] + got_ref[...]
        xs = backward(y_ref[...], arr, w_ref, (uh_ref[...], ul_ref[...]), cols_ref[...], n, lines)
        x = jnp.concatenate(xs, 0)
        x_ref[...] = x
        d_ref[...] = prev_ref[...] - x
        put_edges(d_ref if last else x_ref, par_ref, outs, n, lx, ly)

    field = start
    change = None
    for sweep in range(SWEEPS):
        got = exchange(sends)
        g, y, ahead = call(
            open_forward,
            [block, block, edge],
            field, *got, par, cols, fh, fl, rhs, lh, ll, w,
            scratch=[pltpu.VMEM((4, rows, width), F32)],
        )
        inc = jnp.zeros((lines, width), F32)
        for k in range(segments - 2):
            recv = lax.ppermute(ahead, "line", [(k, k + 1)])
            inc, ahead = call(next_forward, [edge, edge], g, inc, recv, cols, lh, ll, w)
        recv = lax.ppermute(ahead, "line", [(segments - 2, segments - 1)])
        y, behind = call(turn, [block, edge], g, inc, recv, cols, lh, ll, uh, ul, w)
        arr = jnp.zeros((lines, width), F32)
        for k in range(segments - 2):
            recv = lax.ppermute(behind, "line", [(segments - 1 - k, segments - 2 - k)])
            arr, behind = call(next_backward, [edge, edge], y, arr, recv, cols, uh, ul, w)
        recv = lax.ppermute(behind, "line", [(1, 0)])
        out = call(
            functools.partial(close_backward, sweep == SWEEPS - 1),
            [block, block] + edges4,
            y, arr, recv, field, par, cols, uh, ul, w,
        )
        field, change, sends = out[0], out[1], out[2:]

    got = exchange(sends)

    def restrict(x_ref, a, b, c, d, par_ref, cols_ref, fh_ref, fl_ref, rh_ref, rl_ref, lane_ref, res_ref, part_ref, near):
        cols = cols_ref[...]
        res = tangential(x_ref, (a, b, c, d), par_ref, cols, (fh_ref, fl_ref), near, n, lx, ly)
        res_ref[...] = res
        proj = times(res, (rh_ref[...], rl_ref[...]))
        part = lax.broadcasted_iota(jnp.int32, (rows, width), 1) // cb
        proj = jnp.where(part.astype(F32) == cols[:, 19:20], proj, 0.0)
        hit = lax.broadcasted_iota(jnp.int32, (agg_rows, rows), 0).astype(F32)
        hit = jnp.where(hit == lane_ref[0:1, :], 1.0, 0.0).astype(BF16)
        hi, lo = halves(proj)
        part_ref[...] = nn(hit, hi) + nn(hit, lo)

    residual, partial = call(
        restrict,
        [block, ((agg_rows, width), F32)],
        change, *got, par, cols, fh, fl, rh, rl, agg_lane,
        scratch=[pltpu.VMEM((4, rows, width), F32)],
    )
    parts = lax.all_to_all(partial.reshape(owners, owned_rows, width), "ty", 0, 0, tiled=True)

    def solve_coarse(parts_ref, ch_ref, cl_ref, up_ref):
        sums = parts_ref[0]
        for k in range(1, owners):
            sums = sums + parts_ref[k]
        hi, lo = halves(sums)
        zero = jnp.zeros((8 - owned_rows, width), BF16)
        hi, lo = jnp.concatenate([hi, zero], 0), jnp.concatenate([lo, zero], 0)
        both = jnp.concatenate([hi, lo], 0)
        out = nt(both, ch_ref[...])
        out = out[:8] + out[8:] + nt(both, cl_ref[...])[:8]
        row = lax.broadcasted_iota(jnp.int32, (8, width), 0)
        acc = jnp.zeros((8, width), F32)
        for k in range(owned_rows):
            acc = acc + jnp.where(row == k, out[:, k * width : (k + 1) * width], 0.0)
        for k in range(owners):
            up_ref[k] = acc[:owned_rows]

    (copies,) = call(solve_coarse, [((owners, owned_rows, width), F32)], parts, ch, cl)
    update = lax.all_to_all(copies, "ty", 0, 0, tiled=True)

    def correct(up_ref, x_ref, cols_ref, rh_ref, rl_ref, out_ref):
        cols = cols_ref[...]
        hit = lax.broadcasted_iota(jnp.int32, (rows, agg_rows), 1).astype(F32)
        hit = jnp.where(hit == cols[:, 18:19], 1.0, 0.0).astype(BF16)
        hi, lo = halves(up_ref[...])
        picked = nn(hit, hi) + nn(hit, lo)
        part = lax.broadcasted_iota(jnp.int32, (rows, width), 1) // cb
        picked = jnp.where(part.astype(F32) == cols[:, 19:20], picked, 0.0)
        out_ref[...] = x_ref[...] + times(picked, (rh_ref[...], rl_ref[...]), nn)

    (corrected,) = call(correct, [block], update.reshape(agg_rows, width), field, cols, rh, rl)
    return corrected.reshape(right_side.shape), residual.reshape(right_side.shape)


def solution(mesh):
    in_specs = (
        P("line", "tx", "ty", None),
        P("line", "tx", "ty", None),
        P("line", "tx", "ty", None, None),
        P("line", "tx", "ty"),
        P("line", "tx", "ty"),
        P(),
        P(),
        P(),
        P(None, "line", "tx", "ty"),
        P(None, "line", "tx", "ty"),
        P("line", "tx", "ty"),
        P(),
        P("line", "tx", "ty", None, None),
    )
    out_specs = (P("line", "tx", "ty", None), P("line", "tx", "ty", None))
    return jax.shard_map(body, mesh=mesh, in_specs=in_specs, out_specs=out_specs, check_vma=False)
```

```python
import functools

import jax
import jax.numpy as jnp
from jax import lax
from jax.experimental import pallas as pl
from jax.experimental.pallas import tpu as pltpu
from jax.sharding import PartitionSpec as P

SWEEPS = 2
F32 = jnp.float32
BF16 = jnp.bfloat16
SPEC = pl.BlockSpec(memory_space=pltpu.VMEM)


def call(kernel, outs, *args, scratch=(), whole=0):
    return pl.pallas_call(
        kernel,
        in_specs=[pl.BlockSpec(memory_space=pltpu.HBM)] * whole + [SPEC] * (len(args) - whole),
        out_specs=[SPEC] * len(outs),
        out_shape=[pltpu.VMEM(s, d) for s, d in outs],
        scratch_shapes=list(scratch),
        compiler_params=pltpu.CompilerParams(vmem_limit_bytes=24 << 20),
    )(
        *[pltpu.with_memory_space_constraint(a, pltpu.HBM) for a in args[:whole]],
        *[pltpu.with_memory_space_constraint(a, pltpu.VMEM) for a in args[whole:]],
    )


def halves(v):
    hi = v.astype(BF16)
    return hi, (v - hi.astype(F32)).astype(BF16)


def nt(a, b):
    return lax.dot_general(a, b, (((1,), (1,)), ((), ())), preferred_element_type=F32)


def nn(a, b):
    return lax.dot_general(a, b, (((1,), (0,)), ((), ())), preferred_element_type=F32)


def times(v, m, dot=nt):
    n = v.shape[0]
    hi, lo = halves(v)
    both = dot(jnp.concatenate([hi, lo], 0), m[0])
    return both[:n] + both[n:] + dot(hi, m[1])


def each_line(v, weights, lines):
    hi, lo = halves(v)
    out = nt(jnp.concatenate([hi, lo], 0), weights)
    row = lax.broadcasted_iota(jnp.int32, (2 * lines, 128), 0)
    row = jnp.where(row >= lines, row - lines, row)
    acc = jnp.zeros((2 * lines, 128), F32)
    for l in range(lines):
        acc = acc + jnp.where(row == l, out[:, l * 128 : (l + 1) * 128], 0.0)
    return acc[:lines] + acc[lines:]


def forward(g, inc, w_ref, low, cols, n, lines):
    carry, ys = inc, []
    for i in range(n):
        at = slice(i * lines, (i + 1) * lines)
        inner = g[at] - cols[at, 16:17] * times(carry, low)
        carry = each_line(inner, w_ref[i * lines * 128 : (i + 1) * lines * 128, :], lines)
        ys.append(carry)
    return ys


def backward(y, arr, w_ref, upp, cols, n, lines):
    carry, xs = arr, [None] * n
    for i in reversed(range(n)):
        at = slice(i * lines, (i + 1) * lines)
        inner = cols[at, 17:18] * times(carry, upp)
        carry = y[at] - each_line(inner, w_ref[i * lines * 128 : (i + 1) * lines * 128, :], lines)
        xs[i] = carry
    return xs


def is_even(axis):
    return lax.axis_index(axis) % 2 == 0


def put_edges(x_ref, outs, n, lx, ly):
    a_ref, b_ref, c_ref, d_ref = outs
    lines = lx * ly
    first = jnp.concatenate([x_ref[i * lines : i * lines + ly, :] for i in range(n)], 0)
    last = jnp.concatenate([x_ref[(i + 1) * lines - ly : (i + 1) * lines, :] for i in range(n)], 0)
    even = is_even("tx")
    a_ref[...] = jnp.where(even, last, first)
    b_ref[...] = jnp.where(even, first, last)
    first = x_ref[pl.ds(0, n * lx, stride=ly), :]
    last = x_ref[pl.ds(ly - 1, n * lx, stride=ly), :]
    even = is_even("ty")
    c_ref[...] = jnp.where(even, last, first)
    d_ref[...] = jnp.where(even, first, last)


def tangential(x_ref, got, cols, blocks, near, n, lx, ly):
    lines = lx * ly
    x = x_ref[...]
    even = is_even("tx")
    b, c, d, a = (r[...] for r in got)
    below, above = jnp.where(even, b, a), jnp.where(even, a, b)
    near[0] = pltpu.roll(x, ly, 0)
    near[1] = pltpu.roll(x, n * lines - ly, 0)
    for i in range(n):
        near[0, i * lines : i * lines + ly, :] = below[i * ly : (i + 1) * ly]
        near[1, (i + 1) * lines - ly : (i + 1) * lines, :] = above[i * ly : (i + 1) * ly]
    even = is_even("ty")
    below, above = jnp.where(even, d, c), jnp.where(even, c, d)
    row = lax.broadcasted_iota(jnp.int32, x.shape, 0) % ly
    near[2] = pltpu.roll(x, 1, 0)
    near[3] = pltpu.roll(x, n * lines - 1, 0)
    for q in range(n * lx):
        near[2, q * ly : q * ly + 1, :] = below[q : q + 1]
        near[3, q * ly + ly - 1 : q * ly + ly, :] = above[q : q + 1]
    total = jnp.zeros(x.shape, F32)
    beside = [near[s] for s in range(4)]
    for k in range(4):
        mixed = sum(cols[:, 4 * s + k : 4 * s + k + 1] * beside[s] for s in range(4))
        total = total + times(mixed, (blocks[0][k], blocks[1][k]))
    return total


def swaps(count, start):
    return [
        pair
        for i in range(start, count - 1, 2)
        for pair in ((i, i + 1), (i + 1, i))
    ]


def exchange(sends):
    nx, ny = lax.axis_size("tx"), lax.axis_size("ty")
    a, b, c, d = sends
    b = lax.ppermute(b, "tx", swaps(nx, 1))
    c = lax.ppermute(c, "ty", swaps(ny, 0))
    d = lax.ppermute(d, "ty", swaps(ny, 1))
    a = lax.ppermute(a, "tx", swaps(nx, 0))
    return b, c, d, a


def body(
    right_side,
    start_field,
    line_inverse,
    lower_scale,
    upper_scale,
    lower_block,
    upper_block,
    face_blocks,
    face_kind,
    face_scale,
    agglomerate,
    restriction,
    coarse_inverse,
):
    n, lx, ly, width = right_side.shape
    lines, rows, cb = lx * ly, n * lx * ly, restriction.shape[0]
    quarter = width // cb
    segments, owners = lax.axis_size("line"), lax.axis_size("ty")
    owned_rows = coarse_inverse.shape[2] // quarter
    agg_rows = owned_rows * owners
    rhs = right_side.reshape(rows, width)
    start = start_field.reshape(rows, width)
    w = line_inverse.reshape(rows * width, width)

    block, edge = ((rows, width), F32), ((lines, width), F32)
    half, half4 = ((width, width), BF16), ((4, width, width), BF16)
    edges4 = [((n * ly, width), F32)] * 2 + [((n * lx, width), F32)] * 2

    def first_edges(x_ref, *outs):
        put_edges(x_ref, outs, n, lx, ly)

    sends = call(first_edges, edges4, start)

    raw = (
        w,
        lower_block,
        upper_block,
        face_blocks,
        restriction,
        coarse_inverse.reshape(owned_rows * width, cb),
        face_kind,
        face_scale,
        lower_scale,
        upper_scale,
        agglomerate,
    )

    def prepare(*refs):
        outs = refs[len(raw) : len(raw) + 13]
        held, sems = refs[len(raw) + 13 : -1], refs[-1]
        copies = [
            pltpu.make_async_copy(src, dst, sems.at[k])
            for k, (src, dst) in enumerate(zip(refs, (outs[10], *held)))
        ]
        for copy in copies:
            copy.start()
        for copy in copies[1:]:
            copy.wait()
        l_ref, u_ref, f_ref, r_ref, c_ref, kind_ref, face_ref, low_ref, up_ref, agg_ref = held
        for k, src in enumerate((l_ref, u_ref, f_ref)):
            outs[2 * k][...], outs[2 * k + 1][...] = halves(src[...])
        outs[6][...], outs[7][...] = halves(jnp.concatenate([r_ref[...]] * quarter, 0))
        lane = lax.broadcasted_iota(jnp.int32, (cb, width), 1) % cb
        wide = (lane == lax.broadcasted_iota(jnp.int32, (cb, width), 0)).astype(F32).astype(BF16)
        part = (lax.broadcasted_iota(jnp.int32, (owned_rows * width, width), 0) // cb) % quarter
        mine = part == lax.broadcasted_iota(jnp.int32, (owned_rows * width, width), 1) // cb
        for k, piece in enumerate(halves(c_ref[...])):
            outs[8 + k][...] = jnp.where(mine, nn(piece, wide), 0.0).astype(BF16)
        groups = rows // ly
        row = lax.broadcasted_iota(jnp.int32, (rows, groups), 0)
        up = (row // ly == lax.broadcasted_iota(jnp.int32, (rows, groups), 1)).astype(F32).astype(BF16)
        row = lax.broadcasted_iota(jnp.int32, (rows, ly), 0)
        own = row % ly == lax.broadcasted_iota(jnp.int32, (rows, ly), 1)

        def column(ref, *at):
            src = jnp.concatenate([ref[(*at, i)] for i in range(n)], 0).astype(F32)
            hi, lo = halves(src)
            return jnp.sum(jnp.where(own, nn(up, hi) + nn(up, lo), 0.0), axis=1, keepdims=True)

        agg = column(agg_ref).astype(jnp.int32)
        row_of = (agg // quarter).astype(F32)
        listed = []
        for side in range(4):
            kind, face = column(kind_ref, side), column(face_ref, side)
            listed += [jnp.where(kind == float(k), face, 0.0) for k in range(4)]
        listed += [column(low_ref), column(up_ref), row_of, (agg % quarter).astype(F32)]
        lane = lax.broadcasted_iota(jnp.int32, (rows, width), 1)
        cols = jnp.zeros((rows, width), F32)
        for k, value in enumerate(listed):
            cols = jnp.where(lane == k, value, cols)
        outs[11][...] = cols
        square = lax.broadcasted_iota(jnp.int32, (rows, rows), 0) == lax.broadcasted_iota(jnp.int32, (rows, rows), 1)
        across = jnp.sum(jnp.where(square, row_of, 0.0), axis=0, keepdims=True)
        outs[12][...] = jnp.broadcast_to(across, (8, rows))
        copies[0].wait()

    lh, ll, uh, ul, fh, fl, rh, rl, ch, cl, w, cols, agg_lane = call(
        prepare,
        [half, half, half, half, half4, half4, half, half]
        + [((owned_rows * width, width), BF16)] * 2
        + [((rows * width, width), BF16), block, ((8, rows), F32)],
        *raw,
        scratch=[pltpu.VMEM(a.shape, a.dtype) for a in raw[1:]]
        + [pltpu.SemaphoreType.DMA((len(raw),))],
        whole=len(raw),
    )

    def open_forward(x_ref, a, b, c, d, cols_ref, fh_ref, fl_ref, rhs_ref, lh_ref, ll_ref, w_ref, g_ref, y_ref, f_ref, near):
        cols = cols_ref[...]
        total = tangential(x_ref, (a, b, c, d), cols, (fh_ref, fl_ref), near, n, lx, ly)
        g = rhs_ref[...] - total
        g_ref[...] = g
        zero = jnp.zeros((lines, width), F32)
        ys = forward(g, zero, w_ref, (lh_ref[...], ll_ref[...]), cols, n, lines)
        y_ref[...] = jnp.concatenate(ys, 0)
        f_ref[...] = ys[-1]

    def next_forward(g_ref, inc_ref, got_ref, cols_ref, lh_ref, ll_ref, w_ref, sum_ref, f_ref):
        inc = inc_ref[...] + got_ref[...]
        sum_ref[...] = inc
        ys = forward(g_ref[...], inc, w_ref, (lh_ref[...], ll_ref[...]), cols_ref[...], n, lines)
        f_ref[...] = ys[-1]

    def turn(g_ref, inc_ref, got_ref, cols_ref, lh_ref, ll_ref, uh_ref, ul_ref, w_ref, y_ref, x_ref):
        cols = cols_ref[...]
        inc = inc_ref[...] + got_ref[...]
        ys = forward(g_ref[...], inc, w_ref, (lh_ref[...], ll_ref[...]), cols, n, lines)
        y = jnp.concatenate(ys, 0)
        y_ref[...] = y
        zero = jnp.zeros((lines, width), F32)
        xs = backward(y, zero, w_ref, (uh_ref[...], ul_ref[...]), cols, n, lines)
        x_ref[...] = xs[0]

    def next_backward(y_ref, arr_ref, got_ref, cols_ref, uh_ref, ul_ref, w_ref, sum_ref, x_ref):
        arr = arr_ref[...] + got_ref[...]
        sum_ref[...] = arr
        xs = backward(y_ref[...], arr, w_ref, (uh_ref[...], ul_ref[...]), cols_ref[...], n, lines)
        x_ref[...] = xs[0]

    def close_backward(last, y_ref, arr_ref, got_ref, prev_ref, cols_ref, uh_ref, ul_ref, w_ref, x_ref, d_ref, *outs):
        arr = arr_ref[...] + got_ref[...]
        xs = backward(y_ref[...], arr, w_ref, (uh_ref[...], ul_ref[...]), cols_ref[...], n, lines)
        x = jnp.concatenate(xs, 0)
        x_ref[...] = x
        d_ref[...] = prev_ref[...] - x
        put_edges(d_ref if last else x_ref, outs, n, lx, ly)

    field = start
    change = None
    for sweep in range(SWEEPS):
        got = exchange(sends)
        g, y, ahead = call(
            open_forward,
            [block, block, edge],
            field, *got, cols, fh, fl, rhs, lh, ll, w,
            scratch=[pltpu.VMEM((4, rows, width), F32)],
        )
        inc = jnp.zeros((lines, width), F32)
        for k in range(segments - 2):
            recv = lax.ppermute(ahead, "line", [(k, k + 1)])
            inc, ahead = call(next_forward, [edge, edge], g, inc, recv, cols, lh, ll, w)
        recv = lax.ppermute(ahead, "line", [(segments - 2, segments - 1)])
        y, behind = call(turn, [block, edge], g, inc, recv, cols, lh, ll, uh, ul, w)
        arr = jnp.zeros((lines, width), F32)
        for k in range(segments - 2):
            recv = lax.ppermute(behind, "line", [(segments - 1 - k, segments - 2 - k)])
            arr, behind = call(next_backward, [edge, edge], y, arr, recv, cols, uh, ul, w)
        recv = lax.ppermute(behind, "line", [(1, 0)])
        out = call(
            functools.partial(close_backward, sweep == SWEEPS - 1),
            [block, block] + edges4,
            y, arr, recv, field, cols, uh, ul, w,
        )
        field, change, sends = out[0], out[1], out[2:]

    got = exchange(sends)

    def restrict(x_ref, a, b, c, d, cols_ref, fh_ref, fl_ref, rh_ref, rl_ref, lane_ref, res_ref, part_ref, near):
        cols = cols_ref[...]
        res = tangential(x_ref, (a, b, c, d), cols, (fh_ref, fl_ref), near, n, lx, ly)
        res_ref[...] = res
        proj = times(res, (rh_ref[...], rl_ref[...]))
        part = lax.broadcasted_iota(jnp.int32, (rows, width), 1) // cb
        proj = jnp.where(part.astype(F32) == cols[:, 19:20], proj, 0.0)
        hit = lax.broadcasted_iota(jnp.int32, (agg_rows, rows), 0).astype(F32)
        hit = jnp.where(hit == lane_ref[0:1, :], 1.0, 0.0).astype(BF16)
        hi, lo = halves(proj)
        part_ref[...] = nn(hit, hi) + nn(hit, lo)

    residual, partial = call(
        restrict,
        [block, ((agg_rows, width), F32)],
        change, *got, cols, fh, fl, rh, rl, agg_lane,
        scratch=[pltpu.VMEM((4, rows, width), F32)],
    )
    parts = lax.all_to_all(partial.reshape(owners, owned_rows, width), "ty", 0, 0, tiled=True)

    def solve_coarse(parts_ref, ch_ref, cl_ref, up_ref):
        sums = parts_ref[0]
        for k in range(1, owners):
            sums = sums + parts_ref[k]
        hi, lo = halves(sums)
        zero = jnp.zeros((8 - owned_rows, width), BF16)
        hi, lo = jnp.concatenate([hi, zero], 0), jnp.concatenate([lo, zero], 0)
        both = jnp.concatenate([hi, lo], 0)
        out = nt(both, ch_ref[...])
        out = out[:8] + out[8:] + nt(both, cl_ref[...])[:8]
        row = lax.broadcasted_iota(jnp.int32, (8, width), 0)
        acc = jnp.zeros((8, width), F32)
        for k in range(owned_rows):
            acc = acc + jnp.where(row == k, out[:, k * width : (k + 1) * width], 0.0)
        for k in range(owners):
            up_ref[k] = acc[:owned_rows]

    (copies,) = call(solve_coarse, [((owners, owned_rows, width), F32)], parts, ch, cl)
    update = lax.all_to_all(copies, "ty", 0, 0, tiled=True)

    def correct(up_ref, x_ref, cols_ref, rh_ref, rl_ref, out_ref):
        cols = cols_ref[...]
        hit = lax.broadcasted_iota(jnp.int32, (rows, agg_rows), 1).astype(F32)
        hit = jnp.where(hit == cols[:, 18:19], 1.0, 0.0).astype(BF16)
        hi, lo = halves(up_ref[...])
        picked = nn(hit, hi) + nn(hit, lo)
        part = lax.broadcasted_iota(jnp.int32, (rows, width), 1) // cb
        picked = jnp.where(part.astype(F32) == cols[:, 19:20], picked, 0.0)
        out_ref[...] = x_ref[...] + times(picked, (rh_ref[...], rl_ref[...]), nn)

    (corrected,) = call(correct, [block], update.reshape(agg_rows, width), field, cols, rh, rl)
    return corrected.reshape(right_side.shape), residual.reshape(right_side.shape)


def solution(mesh):
    in_specs = (
        P("line", "tx", "ty", None),
        P("line", "tx", "ty", None),
        P("line", "tx", "ty", None, None),
        P("line", "tx", "ty"),
        P("line", "tx", "ty"),
        P(),
        P(),
        P(),
        P(None, "line", "tx", "ty"),
        P(None, "line", "tx", "ty"),
        P("line", "tx", "ty"),
        P(),
        P("line", "tx", "ty", None, None),
    )
    out_specs = (P("line", "tx", "ty", None), P("line", "tx", "ty", None))
    return jax.shard_map(body, mesh=mesh, in_specs=in_specs, out_specs=out_specs, check_vma=False)
```

```python
import functools

import jax
import jax.numpy as jnp
from jax import lax
from jax.experimental import pallas as pl
from jax.experimental.pallas import tpu as pltpu
from jax.sharding import PartitionSpec as P

SWEEPS = 2
F32 = jnp.float32
BF16 = jnp.bfloat16
SPEC = pl.BlockSpec(memory_space=pltpu.VMEM)


def call(kernel, outs, *args, scratch=(), whole=0):
    return pl.pallas_call(
        kernel,
        in_specs=[pl.BlockSpec(memory_space=pltpu.HBM)] * whole + [SPEC] * (len(args) - whole),
        out_specs=[SPEC] * len(outs),
        out_shape=[pltpu.VMEM(s, d) for s, d in outs],
        scratch_shapes=list(scratch),
        compiler_params=pltpu.CompilerParams(vmem_limit_bytes=24 << 20),
    )(
        *[pltpu.with_memory_space_constraint(a, pltpu.HBM) for a in args[:whole]],
        *[pltpu.with_memory_space_constraint(a, pltpu.VMEM) for a in args[whole:]],
    )


def halves(v):
    hi = v.astype(BF16)
    return hi, (v - hi.astype(F32)).astype(BF16)


def nt(a, b):
    return lax.dot_general(a, b, (((1,), (1,)), ((), ())), preferred_element_type=F32)


def nn(a, b):
    return lax.dot_general(a, b, (((1,), (0,)), ((), ())), preferred_element_type=F32)


def times(v, m, dot=nt):
    n = v.shape[0]
    hi, lo = halves(v)
    both = dot(jnp.concatenate([hi, lo], 0), m[0])
    return both[:n] + both[n:] + dot(hi, m[1])


def each_line(v, weights, lines):
    hi, lo = halves(v)
    out = nt(jnp.concatenate([hi, lo], 0), weights)
    row = lax.broadcasted_iota(jnp.int32, (2 * lines, 128), 0)
    row = jnp.where(row >= lines, row - lines, row)
    acc = jnp.zeros((2 * lines, 128), F32)
    for l in range(lines):
        acc = acc + jnp.where(row == l, out[:, l * 128 : (l + 1) * 128], 0.0)
    return acc[:lines] + acc[lines:]


def forward(g, inc, w_ref, low, cols, n, lines):
    carry, ys = inc, []
    for i in range(n):
        at = slice(i * lines, (i + 1) * lines)
        inner = g[at] - cols[at, 16:17] * times(carry, low)
        carry = each_line(inner, w_ref[i * lines * 128 : (i + 1) * lines * 128, :], lines)
        ys.append(carry)
    return ys


def backward(y, arr, w_ref, upp, cols, n, lines):
    carry, xs = arr, [None] * n
    for i in reversed(range(n)):
        at = slice(i * lines, (i + 1) * lines)
        inner = cols[at, 17:18] * times(carry, upp)
        carry = y[at] - each_line(inner, w_ref[i * lines * 128 : (i + 1) * lines * 128, :], lines)
        xs[i] = carry
    return xs


def is_even(axis):
    return lax.axis_index(axis) % 2 == 0


def put_edges(x_ref, outs, n, lx, ly):
    a_ref, b_ref, c_ref, d_ref = outs
    lines = lx * ly
    first = jnp.concatenate([x_ref[i * lines : i * lines + ly, :] for i in range(n)], 0)
    last = jnp.concatenate([x_ref[(i + 1) * lines - ly : (i + 1) * lines, :] for i in range(n)], 0)
    even = is_even("tx")
    a_ref[...] = jnp.where(even, last, first)
    b_ref[...] = jnp.where(even, first, last)
    first = x_ref[pl.ds(0, n * lx, stride=ly), :]
    last = x_ref[pl.ds(ly - 1, n * lx, stride=ly), :]
    even = is_even("ty")
    c_ref[...] = jnp.where(even, last, first)
    d_ref[...] = jnp.where(even, first, last)


def tangential(x_ref, got, cols, blocks, near, n, lx, ly):
    lines = lx * ly
    x = x_ref[...]
    even = is_even("tx")
    b, c, d, a = (r[...] for r in got)
    below, above = jnp.where(even, b, a), jnp.where(even, a, b)
    near[0] = pltpu.roll(x, ly, 0)
    near[1] = pltpu.roll(x, n * lines - ly, 0)
    for i in range(n):
        near[0, i * lines : i * lines + ly, :] = below[i * ly : (i + 1) * ly]
        near[1, (i + 1) * lines - ly : (i + 1) * lines, :] = above[i * ly : (i + 1) * ly]
    even = is_even("ty")
    below, above = jnp.where(even, d, c), jnp.where(even, c, d)
    row = lax.broadcasted_iota(jnp.int32, x.shape, 0) % ly
    near[2] = pltpu.roll(x, 1, 0)
    near[3] = pltpu.roll(x, n * lines - 1, 0)
    for q in range(n * lx):
        near[2, q * ly : q * ly + 1, :] = below[q : q + 1]
        near[3, q * ly + ly - 1 : q * ly + ly, :] = above[q : q + 1]
    total = jnp.zeros(x.shape, F32)
    beside = [near[s] for s in range(4)]
    for k in range(4):
        mixed = sum(cols[:, 4 * s + k : 4 * s + k + 1] * beside[s] for s in range(4))
        total = total + times(mixed, (blocks[0][k], blocks[1][k]))
    return total


def each_line_pair(v, high, low, lines):
    hi, lo = halves(v)
    both = nt(jnp.concatenate([hi, lo], 0), high)
    out = both[:lines] + both[lines:] + nt(hi, low)
    row = lax.broadcasted_iota(jnp.int32, (lines, 128), 0)
    acc = jnp.zeros((lines, 128), F32)
    for l in range(lines):
        acc = acc + jnp.where(row == l, out[:, l * 128 : (l + 1) * 128], 0.0)
    return acc


def advance(prev, out, mat, w_ref, cols_ref, col, i, lines, base=None):
    group = lines // 2
    stacked = jnp.concatenate([mat[0], mat[1]], 0)

    def some(t, _):
        for j in range(group):
            l = t * group + j
            if prev is None:
                xh, xl = mat
            else:
                hi, lo = halves(prev[l])
                both = nn(stacked, jnp.concatenate([hi, lo], 1))
                xh, xl = halves(both[:128, :128] + both[:128, 128:] + both[128:, :128])
            at = i * lines + l
            w = w_ref[pl.ds(pl.multiple_of(at * 128, 128), 128), :]
            y = nn(w, jnp.concatenate([xh, xl], 1))
            y = (y[:, :128] + y[:, 128:]) * cols_ref[pl.ds(at, 1), col : col + 1]
            out[l] = -y if base is None else base[l] - y
        return 0

    lax.fori_loop(0, lines // group, some, 0)


def put_halves(src, high, low, lines):
    def one(l, _):
        at = pl.ds(pl.multiple_of(l * 128, 128), 128)
        high[at, :], low[at, :] = halves(src[l])
        return 0

    lax.fori_loop(0, lines, one, 0)


def swaps(count, start):
    return [
        pair
        for i in range(start, count - 1, 2)
        for pair in ((i, i + 1), (i + 1, i))
    ]


def exchange(sends):
    nx, ny = lax.axis_size("tx"), lax.axis_size("ty")
    a, b, c, d = sends
    b = lax.ppermute(b, "tx", swaps(nx, 1))
    c = lax.ppermute(c, "ty", swaps(ny, 0))
    d = lax.ppermute(d, "ty", swaps(ny, 1))
    a = lax.ppermute(a, "tx", swaps(nx, 0))
    return b, c, d, a


def body(
    right_side,
    start_field,
    line_inverse,
    lower_scale,
    upper_scale,
    lower_block,
    upper_block,
    face_blocks,
    face_kind,
    face_scale,
    agglomerate,
    restriction,
    coarse_inverse,
):
    n, lx, ly, width = right_side.shape
    lines, rows, cb = lx * ly, n * lx * ly, restriction.shape[0]
    quarter = width // cb
    segments, owners = lax.axis_size("line"), lax.axis_size("ty")
    owned_rows = coarse_inverse.shape[2] // quarter
    agg_rows = owned_rows * owners
    rhs = right_side.reshape(rows, width)
    start = start_field.reshape(rows, width)
    w = line_inverse.reshape(rows * width, width)

    block, edge = ((rows, width), F32), ((lines, width), F32)
    half, half4 = ((width, width), BF16), ((4, width, width), BF16)
    edges4 = [((n * ly, width), F32)] * 2 + [((n * lx, width), F32)] * 2

    def first_edges(x_ref, *outs):
        put_edges(x_ref, outs, n, lx, ly)

    sends = call(first_edges, edges4, start)

    raw = (
        w,
        lower_block,
        upper_block,
        face_blocks,
        restriction,
        coarse_inverse.reshape(owned_rows * width, cb),
        face_kind,
        face_scale,
        lower_scale,
        upper_scale,
        agglomerate,
    )

    def prepare(*refs):
        outs = refs[len(raw) : len(raw) + 13]
        held, sems = refs[len(raw) + 13 : -1], refs[-1]
        copies = [
            pltpu.make_async_copy(src, dst, sems.at[k])
            for k, (src, dst) in enumerate(zip(refs, (outs[10], *held)))
        ]
        for copy in copies:
            copy.start()
        for copy in copies[1:]:
            copy.wait()
        l_ref, u_ref, f_ref, r_ref, c_ref, kind_ref, face_ref, low_ref, up_ref, agg_ref = held
        for k, src in enumerate((l_ref, u_ref, f_ref)):
            outs[2 * k][...], outs[2 * k + 1][...] = halves(src[...])
        outs[6][...], outs[7][...] = halves(jnp.concatenate([r_ref[...]] * quarter, 0))
        lane = lax.broadcasted_iota(jnp.int32, (cb, width), 1) % cb
        wide = (lane == lax.broadcasted_iota(jnp.int32, (cb, width), 0)).astype(F32).astype(BF16)
        part = (lax.broadcasted_iota(jnp.int32, (owned_rows * width, width), 0) // cb) % quarter
        mine = part == lax.broadcasted_iota(jnp.int32, (owned_rows * width, width), 1) // cb
        for k, piece in enumerate(halves(c_ref[...])):
            outs[8 + k][...] = jnp.where(mine, nn(piece, wide), 0.0).astype(BF16)
        groups = rows // ly
        row = lax.broadcasted_iota(jnp.int32, (rows, groups), 0)
        up = (row // ly == lax.broadcasted_iota(jnp.int32, (rows, groups), 1)).astype(F32).astype(BF16)
        row = lax.broadcasted_iota(jnp.int32, (rows, ly), 0)
        own = row % ly == lax.broadcasted_iota(jnp.int32, (rows, ly), 1)

        def column(ref, *at):
            src = jnp.concatenate([ref[(*at, i)] for i in range(n)], 0).astype(F32)
            hi, lo = halves(src)
            return jnp.sum(jnp.where(own, nn(up, hi) + nn(up, lo), 0.0), axis=1, keepdims=True)

        agg = column(agg_ref).astype(jnp.int32)
        row_of = (agg // quarter).astype(F32)
        listed = []
        for side in range(4):
            kind, face = column(kind_ref, side), column(face_ref, side)
            listed += [jnp.where(kind == float(k), face, 0.0) for k in range(4)]
        listed += [column(low_ref), column(up_ref), row_of, (agg % quarter).astype(F32)]
        lane = lax.broadcasted_iota(jnp.int32, (rows, width), 1)
        cols = jnp.zeros((rows, width), F32)
        for k, value in enumerate(listed):
            cols = jnp.where(lane == k, value, cols)
        outs[11][...] = cols
        square = lax.broadcasted_iota(jnp.int32, (rows, rows), 0) == lax.broadcasted_iota(jnp.int32, (rows, rows), 1)
        across = jnp.sum(jnp.where(square, row_of, 0.0), axis=0, keepdims=True)
        outs[12][...] = jnp.broadcast_to(across, (8, rows))
        copies[0].wait()

    lh, ll, uh, ul, fh, fl, rh, rl, ch, cl, w, cols, agg_lane = call(
        prepare,
        [half, half, half, half, half4, half4, half, half]
        + [((owned_rows * width, width), BF16)] * 2
        + [((rows * width, width), BF16), block, ((8, rows), F32)],
        *raw,
        scratch=[pltpu.VMEM(a.shape, a.dtype) for a in raw[1:]]
        + [pltpu.SemaphoreType.DMA((len(raw),))],
        whole=len(raw),
    )

    def open_forward(x_ref, a, b, c, d, cols_ref, fh_ref, fl_ref, rhs_ref, lh_ref, ll_ref, w_ref, g_ref, y_ref, f_ref, near):
        cols = cols_ref[...]
        total = tangential(x_ref, (a, b, c, d), cols, (fh_ref, fl_ref), near, n, lx, ly)
        g = rhs_ref[...] - total
        g_ref[...] = g
        zero = jnp.zeros((lines, width), F32)
        ys = forward(g, zero, w_ref, (lh_ref[...], ll_ref[...]), cols, n, lines)
        y_ref[...] = jnp.concatenate(ys, 0)
        f_ref[...] = ys[-1]

    def forward_map(after_ref, cols_ref, lh_ref, ll_ref, w_ref, high, low, one, two):
        pos = lax.axis_index("line")

        @pl.when((pos > 0) & (pos < segments - 1))
        def _():
            mat, prev = (lh_ref[...], ll_ref[...]), None
            for i in range(n):
                now = (one, two)[i % 2]
                advance(prev, now, mat, w_ref, cols_ref, 16, i, lines)
                prev = now
            put_halves(prev, high, low, lines)

    def backward_map(after_ref, cols_ref, uh_ref, ul_ref, w_ref, high, low, one, two):
        pos = lax.axis_index("line")

        @pl.when((pos > 0) & (pos < segments - 1))
        def _():
            mat, prev = (uh_ref[...], ul_ref[...]), None
            for i in reversed(range(n)):
                now = (one, two)[i % 2]
                advance(prev, now, mat, w_ref, cols_ref, 17, i, lines)
                prev = now
            put_halves(prev, high, low, lines)

    def turn_map(after_ref, cols_ref, lh_ref, ll_ref, uh_ref, ul_ref, w_ref, high, low, steps, one, two):
        @pl.when(lax.axis_index("line") == segments - 1)
        def _():
            mat, prev = (lh_ref[...], ll_ref[...]), None
            for i in range(n):
                advance(prev, steps.at[i], mat, w_ref, cols_ref, 16, i, lines)
                prev = steps.at[i]
            mat = (uh_ref[...], ul_ref[...])
            for i in reversed(range(n - 1)):
                now = (one, two)[i % 2]
                advance(prev, now, mat, w_ref, cols_ref, 17, i, lines, steps.at[i])
                prev = now
            put_halves(prev, high, low, lines)

    def next_forward(first_ref, inc_ref, got_ref, high, low, sum_ref, f_ref):
        inc = inc_ref[...] + got_ref[...]
        sum_ref[...] = inc
        f_ref[...] = first_ref[...] + each_line_pair(inc, high[...], low[...], lines)

    def local_back(after_ref, y_ref, cols_ref, uh_ref, ul_ref, w_ref, x_ref):
        zero = jnp.zeros((lines, width), F32)
        x_ref[...] = backward(y_ref[...], zero, w_ref, (uh_ref[...], ul_ref[...]), cols_ref[...], n, lines)[0]

    def turn(local_ref, inc_ref, got_ref, high, low, sum_ref, x_ref):
        inc = inc_ref[...] + got_ref[...]
        sum_ref[...] = inc
        x_ref[...] = local_ref[...] + each_line_pair(inc, high[...], low[...], lines)

    def settle(after_ref, g_ref, inc_ref, cols_ref, lh_ref, ll_ref, uh_ref, ul_ref, w_ref, y_ref, x_ref):
        cols = cols_ref[...]
        ys = forward(g_ref[...], inc_ref[...], w_ref, (lh_ref[...], ll_ref[...]), cols, n, lines)
        y = jnp.concatenate(ys, 0)
        y_ref[...] = y
        zero = jnp.zeros((lines, width), F32)
        x_ref[...] = backward(y, zero, w_ref, (uh_ref[...], ul_ref[...]), cols, n, lines)[0]

    def next_backward(first_ref, arr_ref, got_ref, high, low, sum_ref, x_ref):
        arr = arr_ref[...] + got_ref[...]
        sum_ref[...] = arr
        x_ref[...] = first_ref[...] + each_line_pair(arr, high[...], low[...], lines)

    def close_backward(last, y_ref, arr_ref, got_ref, prev_ref, cols_ref, uh_ref, ul_ref, w_ref, x_ref, d_ref, *outs):
        arr = arr_ref[...] + got_ref[...]
        xs = backward(y_ref[...], arr, w_ref, (uh_ref[...], ul_ref[...]), cols_ref[...], n, lines)
        x = jnp.concatenate(xs, 0)
        x_ref[...] = x
        d_ref[...] = prev_ref[...] - x
        put_edges(d_ref if last else x_ref, outs, n, lx, ly)

    pair = [((lines * width, width), BF16)] * 2
    two = [pltpu.VMEM((lines, width, width), F32)] * 2
    field = start
    change = None
    for sweep in range(SWEEPS):
        got = exchange(sends)
        g, y, ahead = call(
            open_forward,
            [block, block, edge],
            field, *got, cols, fh, fl, rhs, lh, ll, w,
            scratch=[pltpu.VMEM((4, rows, width), F32)],
        )
        first = ahead
        inc = jnp.zeros((lines, width), F32)
        for k in range(segments - 2):
            recv = lax.ppermute(ahead, "line", [(k, k + 1)])
            if sweep == 0 and k == 0:
                maps = [call(forward_map, pair, ahead, cols, lh, ll, w, scratch=two)]
            inc, ahead = call(next_forward, [edge, edge], first, inc, recv, *maps[0])
            if k == 0:
                local = call(local_back, [edge], ahead, y, cols, uh, ul, w)[0]
                if sweep == 0:
                    steps = [pltpu.VMEM((n, lines, width, width), F32)]
                    maps.append(call(turn_map, pair, ahead, cols, lh, ll, uh, ul, w, scratch=steps + two))
        recv = lax.ppermute(ahead, "line", [(segments - 2, segments - 1)])
        if sweep == 0:
            maps.append(call(backward_map, pair, ahead, cols, uh, ul, w, scratch=two))
        inc, behind = call(turn, [edge, edge], local, inc, recv, *maps[1])
        arr = jnp.zeros((lines, width), F32)
        for k in range(segments - 2):
            recv = lax.ppermute(behind, "line", [(segments - 1 - k, segments - 2 - k)])
            if k == 0:
                y, first = call(settle, [block, edge], behind, g, inc, cols, lh, ll, uh, ul, w)
            arr, behind = call(next_backward, [edge, edge], first, arr, recv, *maps[2])
        recv = lax.ppermute(behind, "line", [(1, 0)])
        out = call(
            functools.partial(close_backward, sweep == SWEEPS - 1),
            [block, block] + edges4,
            y, arr, recv, field, cols, uh, ul, w,
        )
        field, change, sends = out[0], out[1], out[2:]

    got = exchange(sends)

    def restrict(x_ref, a, b, c, d, cols_ref, fh_ref, fl_ref, rh_ref, rl_ref, lane_ref, res_ref, part_ref, near):
        cols = cols_ref[...]
        res = tangential(x_ref, (a, b, c, d), cols, (fh_ref, fl_ref), near, n, lx, ly)
        res_ref[...] = res
        proj = times(res, (rh_ref[...], rl_ref[...]))
        part = lax.broadcasted_iota(jnp.int32, (rows, width), 1) // cb
        proj = jnp.where(part.astype(F32) == cols[:, 19:20], proj, 0.0)
        hit = lax.broadcasted_iota(jnp.int32, (agg_rows, rows), 0).astype(F32)
        hit = jnp.where(hit == lane_ref[0:1, :], 1.0, 0.0).astype(BF16)
        hi, lo = halves(proj)
        part_ref[...] = nn(hit, hi) + nn(hit, lo)

    residual, partial = call(
        restrict,
        [block, ((agg_rows, width), F32)],
        change, *got, cols, fh, fl, rh, rl, agg_lane,
        scratch=[pltpu.VMEM((4, rows, width), F32)],
    )
    parts = lax.all_to_all(partial.reshape(owners, owned_rows, width), "ty", 0, 0, tiled=True)

    def solve_coarse(parts_ref, ch_ref, cl_ref, up_ref):
        sums = parts_ref[0]
        for k in range(1, owners):
            sums = sums + parts_ref[k]
        hi, lo = halves(sums)
        zero = jnp.zeros((8 - owned_rows, width), BF16)
        hi, lo = jnp.concatenate([hi, zero], 0), jnp.concatenate([lo, zero], 0)
        both = jnp.concatenate([hi, lo], 0)
        out = nt(both, ch_ref[...])
        out = out[:8] + out[8:] + nt(both, cl_ref[...])[:8]
        row = lax.broadcasted_iota(jnp.int32, (8, width), 0)
        acc = jnp.zeros((8, width), F32)
        for k in range(owned_rows):
            acc = acc + jnp.where(row == k, out[:, k * width : (k + 1) * width], 0.0)
        for k in range(owners):
            up_ref[k] = acc[:owned_rows]

    (copies,) = call(solve_coarse, [((owners, owned_rows, width), F32)], parts, ch, cl)
    update = lax.all_to_all(copies, "ty", 0, 0, tiled=True)

    def correct(up_ref, x_ref, cols_ref, rh_ref, rl_ref, out_ref):
        cols = cols_ref[...]
        hit = lax.broadcasted_iota(jnp.int32, (rows, agg_rows), 1).astype(F32)
        hit = jnp.where(hit == cols[:, 18:19], 1.0, 0.0).astype(BF16)
        hi, lo = halves(up_ref[...])
        picked = nn(hit, hi) + nn(hit, lo)
        part = lax.broadcasted_iota(jnp.int32, (rows, width), 1) // cb
        picked = jnp.where(part.astype(F32) == cols[:, 19:20], picked, 0.0)
        out_ref[...] = x_ref[...] + times(picked, (rh_ref[...], rl_ref[...]), nn)

    (corrected,) = call(correct, [block], update.reshape(agg_rows, width), field, cols, rh, rl)
    return corrected.reshape(right_side.shape), residual.reshape(right_side.shape)


def solution(mesh):
    in_specs = (
        P("line", "tx", "ty", None),
        P("line", "tx", "ty", None),
        P("line", "tx", "ty", None, None),
        P("line", "tx", "ty"),
        P("line", "tx", "ty"),
        P(),
        P(),
        P(),
        P(None, "line", "tx", "ty"),
        P(None, "line", "tx", "ty"),
        P("line", "tx", "ty"),
        P(),
        P("line", "tx", "ty", None, None),
    )
    out_specs = (P("line", "tx", "ty", None), P("line", "tx", "ty", None))
    return jax.shard_map(body, mesh=mesh, in_specs=in_specs, out_specs=out_specs, check_vma=False)
```

```python
import functools

import jax
import jax.numpy as jnp
from jax import lax
from jax.experimental import pallas as pl
from jax.experimental.pallas import tpu as pltpu
from jax.sharding import PartitionSpec as P

SWEEPS = 2
F32 = jnp.float32
BF16 = jnp.bfloat16
SPEC = pl.BlockSpec(memory_space=pltpu.VMEM)


def call(kernel, outs, *args, scratch=(), whole=0):
    return pl.pallas_call(
        kernel,
        in_specs=[pl.BlockSpec(memory_space=pltpu.HBM)] * whole + [SPEC] * (len(args) - whole),
        out_specs=[SPEC] * len(outs),
        out_shape=[pltpu.VMEM(s, d) for s, d in outs],
        scratch_shapes=list(scratch),
        compiler_params=pltpu.CompilerParams(vmem_limit_bytes=24 << 20),
    )(
        *[pltpu.with_memory_space_constraint(a, pltpu.HBM) for a in args[:whole]],
        *[pltpu.with_memory_space_constraint(a, pltpu.VMEM) for a in args[whole:]],
    )


def halves(v):
    hi = v.astype(BF16)
    return hi, (v - hi.astype(F32)).astype(BF16)


def nt(a, b):
    return lax.dot_general(a, b, (((1,), (1,)), ((), ())), preferred_element_type=F32)


def nn(a, b):
    return lax.dot_general(a, b, (((1,), (0,)), ((), ())), preferred_element_type=F32)


def times(v, m, dot=nt):
    n = v.shape[0]
    hi, lo = halves(v)
    both = dot(jnp.concatenate([hi, lo], 0), m[0])
    return both[:n] + both[n:] + dot(hi, m[1])


def each_line(v, weights, lines):
    hi, lo = halves(v)
    out = nt(jnp.concatenate([hi, lo], 0), weights)
    row = lax.broadcasted_iota(jnp.int32, (2 * lines, 128), 0)
    row = jnp.where(row >= lines, row - lines, row)
    acc = jnp.zeros((2 * lines, 128), F32)
    for l in range(lines):
        acc = acc + jnp.where(row == l, out[:, l * 128 : (l + 1) * 128], 0.0)
    return acc[:lines] + acc[lines:]


def forward(g, inc, w_ref, low, cols, n, lines):
    carry, ys = inc, []
    for i in range(n):
        at = slice(i * lines, (i + 1) * lines)
        inner = g[at] - cols[at, 16:17] * times(carry, low)
        carry = each_line(inner, w_ref[i * lines * 128 : (i + 1) * lines * 128, :], lines)
        ys.append(carry)
    return ys


def backward(y, arr, w_ref, upp, cols, n, lines):
    carry, xs = arr, [None] * n
    for i in reversed(range(n)):
        at = slice(i * lines, (i + 1) * lines)
        inner = cols[at, 17:18] * times(carry, upp)
        carry = y[at] - each_line(inner, w_ref[i * lines * 128 : (i + 1) * lines * 128, :], lines)
        xs[i] = carry
    return xs


def is_even(axis):
    return lax.axis_index(axis) % 2 == 0


def put_edges(x_ref, outs, n, lx, ly):
    a_ref, b_ref, c_ref, d_ref = outs
    lines = lx * ly
    first = jnp.concatenate([x_ref[i * lines : i * lines + ly, :] for i in range(n)], 0)
    last = jnp.concatenate([x_ref[(i + 1) * lines - ly : (i + 1) * lines, :] for i in range(n)], 0)
    even = is_even("tx")
    a_ref[...] = jnp.where(even, last, first)
    b_ref[...] = jnp.where(even, first, last)
    first = x_ref[pl.ds(0, n * lx, stride=ly), :]
    last = x_ref[pl.ds(ly - 1, n * lx, stride=ly), :]
    even = is_even("ty")
    c_ref[...] = jnp.where(even, last, first)
    d_ref[...] = jnp.where(even, first, last)


def tangential(x_ref, got, cols, blocks, near, n, lx, ly):
    lines = lx * ly
    x = x_ref[...]
    even = is_even("tx")
    d, c, b, a = (r[...] for r in got)
    below, above = jnp.where(even, b, a), jnp.where(even, a, b)
    near[0] = pltpu.roll(x, ly, 0)
    near[1] = pltpu.roll(x, n * lines - ly, 0)
    for i in range(n):
        near[0, i * lines : i * lines + ly, :] = below[i * ly : (i + 1) * ly]
        near[1, (i + 1) * lines - ly : (i + 1) * lines, :] = above[i * ly : (i + 1) * ly]
    even = is_even("ty")
    below, above = jnp.where(even, d, c), jnp.where(even, c, d)
    row = lax.broadcasted_iota(jnp.int32, x.shape, 0) % ly
    near[2] = pltpu.roll(x, 1, 0)
    near[3] = pltpu.roll(x, n * lines - 1, 0)
    for q in range(n * lx):
        near[2, q * ly : q * ly + 1, :] = below[q : q + 1]
        near[3, q * ly + ly - 1 : q * ly + ly, :] = above[q : q + 1]
    total = jnp.zeros(x.shape, F32)
    beside = [near[s] for s in range(4)]
    for k in range(4):
        mixed = sum(cols[:, 4 * s + k : 4 * s + k + 1] * beside[s] for s in range(4))
        total = total + times(mixed, (blocks[0][k], blocks[1][k]))
    return total


def each_line_pair(v, high, low, lines):
    hi, lo = halves(v)
    both = nt(jnp.concatenate([hi, lo], 0), high)
    out = both[:lines] + both[lines:] + nt(hi, low)
    row = lax.broadcasted_iota(jnp.int32, (lines, 128), 0)
    acc = jnp.zeros((lines, 128), F32)
    for l in range(lines):
        acc = acc + jnp.where(row == l, out[:, l * 128 : (l + 1) * 128], 0.0)
    return acc


def advance(prev, out, mat, w_ref, cols_ref, col, i, lines, base=None):
    group = lines // 2
    left = jnp.concatenate([mat[0], mat[0], mat[1]], 1)

    def some(t, _):
        for j in range(group):
            l = t * group + j
            if prev is None:
                xh, xl = mat
            else:
                hi, lo = halves(prev[l])
                xh, xl = halves(nn(left, jnp.concatenate([hi, lo, hi], 0)))
            at = i * lines + l
            w = w_ref[pl.ds(pl.multiple_of(at * 128, 128), 128), :]
            y = nn(jnp.concatenate([w, w], 1), jnp.concatenate([xh, xl], 0))
            y = y * cols_ref[pl.ds(at, 1), col : col + 1]
            out[l] = -y if base is None else base[l] - y
        return 0

    lax.fori_loop(0, lines // group, some, 0)


def put_halves(src, high, low, lines):
    def one(l, _):
        at = pl.ds(pl.multiple_of(l * 128, 128), 128)
        high[at, :], low[at, :] = halves(src[l])
        return 0

    lax.fori_loop(0, lines, one, 0)


def swaps(count, start):
    return [
        pair
        for i in range(start, count - 1, 2)
        for pair in ((i, i + 1), (i + 1, i))
    ]


def exchange(sends):
    nx, ny = lax.axis_size("tx"), lax.axis_size("ty")
    a, b, c, d = sends
    d = lax.ppermute(d, "ty", swaps(ny, 1))
    c = lax.ppermute(c, "ty", swaps(ny, 0))
    b = lax.ppermute(b, "tx", swaps(nx, 1))
    a = lax.ppermute(a, "tx", swaps(nx, 0))
    return d, c, b, a


def body(
    right_side,
    start_field,
    line_inverse,
    lower_scale,
    upper_scale,
    lower_block,
    upper_block,
    face_blocks,
    face_kind,
    face_scale,
    agglomerate,
    restriction,
    coarse_inverse,
):
    n, lx, ly, width = right_side.shape
    lines, rows, cb = lx * ly, n * lx * ly, restriction.shape[0]
    quarter = width // cb
    segments, owners = lax.axis_size("line"), lax.axis_size("ty")
    owned_rows = coarse_inverse.shape[2] // quarter
    agg_rows = owned_rows * owners
    rhs = right_side.reshape(rows, width)
    start = start_field.reshape(rows, width)
    w = line_inverse.reshape(rows * width, width)

    block, edge = ((rows, width), F32), ((lines, width), F32)
    half, half4 = ((width, width), BF16), ((4, width, width), BF16)
    edges4 = [((n * ly, width), F32)] * 2 + [((n * lx, width), F32)] * 2

    def first_edges(x_ref, *outs):
        put_edges(x_ref, outs, n, lx, ly)

    sends = call(first_edges, edges4, start)

    raw = (
        w,
        lower_block,
        upper_block,
        face_blocks,
        restriction,
        coarse_inverse.reshape(owned_rows * width, cb),
        face_kind,
        face_scale,
        lower_scale,
        upper_scale,
        agglomerate,
    )

    def prepare(*refs):
        outs = refs[len(raw) : len(raw) + 13]
        held, sems = refs[len(raw) + 13 : -1], refs[-1]
        copies = [
            pltpu.make_async_copy(src, dst, sems.at[k])
            for k, (src, dst) in enumerate(zip(refs, (outs[10], *held)))
        ]
        for copy in copies:
            copy.start()
        for copy in copies[1:]:
            copy.wait()
        l_ref, u_ref, f_ref, r_ref, c_ref, kind_ref, face_ref, low_ref, up_ref, agg_ref = held
        for k, src in enumerate((l_ref, u_ref, f_ref)):
            outs[2 * k][...], outs[2 * k + 1][...] = halves(src[...])
        outs[6][...], outs[7][...] = halves(jnp.concatenate([r_ref[...]] * quarter, 0))
        lane = lax.broadcasted_iota(jnp.int32, (cb, width), 1) % cb
        wide = (lane == lax.broadcasted_iota(jnp.int32, (cb, width), 0)).astype(F32).astype(BF16)
        part = (lax.broadcasted_iota(jnp.int32, (owned_rows * width, width), 0) // cb) % quarter
        mine = part == lax.broadcasted_iota(jnp.int32, (owned_rows * width, width), 1) // cb
        for k, piece in enumerate(halves(c_ref[...])):
            outs[8 + k][...] = jnp.where(mine, nn(piece, wide), 0.0).astype(BF16)
        groups = rows // ly
        row = lax.broadcasted_iota(jnp.int32, (rows, groups), 0)
        up = (row // ly == lax.broadcasted_iota(jnp.int32, (rows, groups), 1)).astype(F32).astype(BF16)
        row = lax.broadcasted_iota(jnp.int32, (rows, ly), 0)
        own = row % ly == lax.broadcasted_iota(jnp.int32, (rows, ly), 1)

        def column(ref, *at):
            src = jnp.concatenate([ref[(*at, i)] for i in range(n)], 0).astype(F32)
            hi, lo = halves(src)
            return jnp.sum(jnp.where(own, nn(up, hi) + nn(up, lo), 0.0), axis=1, keepdims=True)

        agg = column(agg_ref).astype(jnp.int32)
        row_of = (agg // quarter).astype(F32)
        listed = []
        for side in range(4):
            kind, face = column(kind_ref, side), column(face_ref, side)
            listed += [jnp.where(kind == float(k), face, 0.0) for k in range(4)]
        listed += [column(low_ref), column(up_ref), row_of, (agg % quarter).astype(F32)]
        lane = lax.broadcasted_iota(jnp.int32, (rows, width), 1)
        cols = jnp.zeros((rows, width), F32)
        for k, value in enumerate(listed):
            cols = jnp.where(lane == k, value, cols)
        outs[11][...] = cols
        square = lax.broadcasted_iota(jnp.int32, (rows, rows), 0) == lax.broadcasted_iota(jnp.int32, (rows, rows), 1)
        across = jnp.sum(jnp.where(square, row_of, 0.0), axis=0, keepdims=True)
        outs[12][...] = jnp.broadcast_to(across, (8, rows))
        copies[0].wait()

    lh, ll, uh, ul, fh, fl, rh, rl, ch, cl, w, cols, agg_lane = call(
        prepare,
        [half, half, half, half, half4, half4, half, half]
        + [((owned_rows * width, width), BF16)] * 2
        + [((rows * width, width), BF16), block, ((8, rows), F32)],
        *raw,
        scratch=[pltpu.VMEM(a.shape, a.dtype) for a in raw[1:]]
        + [pltpu.SemaphoreType.DMA((len(raw),))],
        whole=len(raw),
    )

    def open_forward(x_ref, a, b, c, d, cols_ref, fh_ref, fl_ref, rhs_ref, lh_ref, ll_ref, w_ref, g_ref, y_ref, f_ref, near):
        cols = cols_ref[...]
        total = tangential(x_ref, (a, b, c, d), cols, (fh_ref, fl_ref), near, n, lx, ly)
        g = rhs_ref[...] - total
        g_ref[...] = g
        zero = jnp.zeros((lines, width), F32)
        ys = forward(g, zero, w_ref, (lh_ref[...], ll_ref[...]), cols, n, lines)
        y_ref[...] = jnp.concatenate(ys, 0)
        f_ref[...] = ys[-1]

    def forward_map(after_ref, cols_ref, lh_ref, ll_ref, w_ref, high, low, one, two):
        pos = lax.axis_index("line")

        @pl.when((pos > 0) & (pos < segments - 1))
        def _():
            mat, prev = (lh_ref[...], ll_ref[...]), None
            for i in range(n):
                now = (one, two)[i % 2]
                advance(prev, now, mat, w_ref, cols_ref, 16, i, lines)
                prev = now
            put_halves(prev, high, low, lines)

    def backward_map(after_ref, cols_ref, uh_ref, ul_ref, w_ref, high, low, one, two):
        pos = lax.axis_index("line")

        @pl.when((pos > 0) & (pos < segments - 1))
        def _():
            mat, prev = (uh_ref[...], ul_ref[...]), None
            for i in reversed(range(n)):
                now = (one, two)[i % 2]
                advance(prev, now, mat, w_ref, cols_ref, 17, i, lines)
                prev = now
            put_halves(prev, high, low, lines)

    def turn_map(after_ref, cols_ref, lh_ref, ll_ref, uh_ref, ul_ref, w_ref, high, low, steps, one, two):
        @pl.when(lax.axis_index("line") == segments - 1)
        def _():
            mat, prev = (lh_ref[...], ll_ref[...]), None
            for i in range(n):
                advance(prev, steps.at[i], mat, w_ref, cols_ref, 16, i, lines)
                prev = steps.at[i]
            mat = (uh_ref[...], ul_ref[...])
            for i in reversed(range(n - 1)):
                now = (one, two)[i % 2]
                advance(prev, now, mat, w_ref, cols_ref, 17, i, lines, steps.at[i])
                prev = now
            put_halves(prev, high, low, lines)

    def chain_forward(stage, g_ref, inc_ref, got_ref, cols_ref, lh_ref, ll_ref, w_ref, sum_ref, f_ref):
        inc = inc_ref[...] + got_ref[...]
        sum_ref[...] = inc

        @pl.when(lax.axis_index("line") == stage)
        def _():
            ys = forward(g_ref[...], inc, w_ref, (lh_ref[...], ll_ref[...]), cols_ref[...], n, lines)
            f_ref[...] = ys[-1]

    def chain_turn(g_ref, inc_ref, got_ref, cols_ref, lh_ref, ll_ref, uh_ref, ul_ref, w_ref, after, after_too, y_ref, x_ref):
        cols = cols_ref[...]
        inc = inc_ref[...] + got_ref[...]
        ys = forward(g_ref[...], inc, w_ref, (lh_ref[...], ll_ref[...]), cols, n, lines)
        for i in range(n):
            y_ref[i * lines : (i + 1) * lines, :] = ys[i]

        @pl.when(lax.axis_index("line") == segments - 1)
        def _():
            zero = jnp.zeros((lines, width), F32)
            x_ref[...] = backward(y_ref[...], zero, w_ref, (uh_ref[...], ul_ref[...]), cols, n, lines)[0]

    def chain_backward(stage, y_ref, arr_ref, got_ref, cols_ref, uh_ref, ul_ref, w_ref, after, after_too, sum_ref, x_ref):
        arr = arr_ref[...] + got_ref[...]
        sum_ref[...] = arr

        @pl.when(lax.axis_index("line") == stage)
        def _():
            xs = backward(y_ref[...], arr, w_ref, (uh_ref[...], ul_ref[...]), cols_ref[...], n, lines)
            x_ref[...] = xs[0]

    def next_forward(first_ref, inc_ref, got_ref, high, low, sum_ref, f_ref):
        inc = inc_ref[...] + got_ref[...]
        sum_ref[...] = inc
        f_ref[...] = first_ref[...] + each_line_pair(inc, high[...], low[...], lines)

    def local_back(after_ref, y_ref, cols_ref, uh_ref, ul_ref, w_ref, x_ref):
        zero = jnp.zeros((lines, width), F32)
        x_ref[...] = backward(y_ref[...], zero, w_ref, (uh_ref[...], ul_ref[...]), cols_ref[...], n, lines)[0]

    def turn(local_ref, inc_ref, got_ref, high, low, sum_ref, x_ref):
        inc = inc_ref[...] + got_ref[...]
        sum_ref[...] = inc
        x_ref[...] = local_ref[...] + each_line_pair(inc, high[...], low[...], lines)

    def settle(after_ref, g_ref, inc_ref, cols_ref, lh_ref, ll_ref, uh_ref, ul_ref, w_ref, y_ref, x_ref):
        cols = cols_ref[...]
        ys = forward(g_ref[...], inc_ref[...], w_ref, (lh_ref[...], ll_ref[...]), cols, n, lines)
        y = jnp.concatenate(ys, 0)
        y_ref[...] = y
        zero = jnp.zeros((lines, width), F32)
        x_ref[...] = backward(y, zero, w_ref, (uh_ref[...], ul_ref[...]), cols, n, lines)[0]

    def next_backward(first_ref, arr_ref, got_ref, high, low, sum_ref, x_ref):
        arr = arr_ref[...] + got_ref[...]
        sum_ref[...] = arr
        x_ref[...] = first_ref[...] + each_line_pair(arr, high[...], low[...], lines)

    def close_backward(last, y_ref, arr_ref, got_ref, prev_ref, cols_ref, uh_ref, ul_ref, w_ref, x_ref, d_ref, *outs):
        arr = arr_ref[...] + got_ref[...]
        xs = backward(y_ref[...], arr, w_ref, (uh_ref[...], ul_ref[...]), cols_ref[...], n, lines)
        x = jnp.concatenate(xs, 0)
        x_ref[...] = x
        d_ref[...] = prev_ref[...] - x
        put_edges(d_ref if last else x_ref, outs, n, lx, ly)

    pair = [((lines * width, width), BF16)] * 2
    two = [pltpu.VMEM((lines, width, width), F32)] * 2
    field = start
    change = None
    for sweep in range(SWEEPS):
        got = exchange(sends)
        g, y, ahead = call(
            open_forward,
            [block, block, edge],
            field, *got, cols, fh, fl, rhs, lh, ll, w,
            scratch=[pltpu.VMEM((4, rows, width), F32)],
        )
        inc = arr = jnp.zeros((lines, width), F32)
        if sweep == 0:
            for k in range(segments - 2):
                recv = lax.ppermute(ahead, "line", [(k, k + 1)])
                step = functools.partial(chain_forward, k + 1)
                inc, ahead = call(step, [edge, edge], g, inc, recv, cols, lh, ll, w)
            recv = lax.ppermute(ahead, "line", [(segments - 2, segments - 1)])
            back = call(backward_map, pair, ahead, cols, uh, ul, w, scratch=two)
            y, behind = call(chain_turn, [block, edge], g, inc, recv, cols, lh, ll, uh, ul, w, *back)
            for k in range(segments - 2):
                recv = lax.ppermute(behind, "line", [(segments - 1 - k, segments - 2 - k)])
                if k == 0:
                    steps = [pltpu.VMEM((n, lines, width, width), F32)]
                    bend = call(turn_map, pair, behind, cols, lh, ll, uh, ul, w, scratch=steps + two)
                if k == segments - 3:
                    fore = call(forward_map, pair, behind, cols, lh, ll, w, scratch=two)
                step = functools.partial(chain_backward, segments - 2 - k)
                made = fore if k == segments - 3 else bend
                arr, behind = call(step, [edge, edge], y, arr, recv, cols, uh, ul, w, *made)
        else:
            first = ahead
            for k in range(segments - 2):
                recv = lax.ppermute(ahead, "line", [(k, k + 1)])
                inc, ahead = call(next_forward, [edge, edge], first, inc, recv, *fore)
                if k == 0:
                    local = call(local_back, [edge], ahead, y, cols, uh, ul, w)[0]
            recv = lax.ppermute(ahead, "line", [(segments - 2, segments - 1)])
            inc, behind = call(turn, [edge, edge], local, inc, recv, *bend)
            for k in range(segments - 2):
                recv = lax.ppermute(behind, "line", [(segments - 1 - k, segments - 2 - k)])
                if k == 0:
                    y, first = call(settle, [block, edge], behind, g, inc, cols, lh, ll, uh, ul, w)
                arr, behind = call(next_backward, [edge, edge], first, arr, recv, *back)
        recv = lax.ppermute(behind, "line", [(1, 0)])
        out = call(
            functools.partial(close_backward, sweep == SWEEPS - 1),
            [block, block] + edges4,
            y, arr, recv, field, cols, uh, ul, w,
        )
        field, change, sends = out[0], out[1], out[2:]

    got = exchange(sends)

    def restrict(x_ref, a, b, c, d, cols_ref, fh_ref, fl_ref, rh_ref, rl_ref, lane_ref, res_ref, part_ref, near):
        cols = cols_ref[...]
        res = tangential(x_ref, (a, b, c, d), cols, (fh_ref, fl_ref), near, n, lx, ly)
        res_ref[...] = res
        proj = times(res, (rh_ref[...], rl_ref[...]))
        part = lax.broadcasted_iota(jnp.int32, (rows, width), 1) // cb
        proj = jnp.where(part.astype(F32) == cols[:, 19:20], proj, 0.0)
        hit = lax.broadcasted_iota(jnp.int32, (agg_rows, rows), 0).astype(F32)
        hit = jnp.where(hit == lane_ref[0:1, :], 1.0, 0.0).astype(BF16)
        hi, lo = halves(proj)
        part_ref[...] = nn(hit, hi) + nn(hit, lo)

    residual, partial = call(
        restrict,
        [block, ((agg_rows, width), F32)],
        change, *got, cols, fh, fl, rh, rl, agg_lane,
        scratch=[pltpu.VMEM((4, rows, width), F32)],
    )
    parts = lax.all_to_all(partial.reshape(owners, owned_rows, width), "ty", 0, 0, tiled=True)

    def solve_coarse(parts_ref, ch_ref, cl_ref, up_ref):
        sums = parts_ref[0]
        for k in range(1, owners):
            sums = sums + parts_ref[k]
        hi, lo = halves(sums)
        zero = jnp.zeros((8 - owned_rows, width), BF16)
        hi, lo = jnp.concatenate([hi, zero], 0), jnp.concatenate([lo, zero], 0)
        both = jnp.concatenate([hi, lo], 0)
        out = nt(both, ch_ref[...])
        out = out[:8] + out[8:] + nt(both, cl_ref[...])[:8]
        row = lax.broadcasted_iota(jnp.int32, (8, width), 0)
        acc = jnp.zeros((8, width), F32)
        for k in range(owned_rows):
            acc = acc + jnp.where(row == k, out[:, k * width : (k + 1) * width], 0.0)
        for k in range(owners):
            up_ref[k] = acc[:owned_rows]

    (copies,) = call(solve_coarse, [((owners, owned_rows, width), F32)], parts, ch, cl)
    update = lax.all_to_all(copies, "ty", 0, 0, tiled=True)

    def correct(up_ref, x_ref, cols_ref, rh_ref, rl_ref, out_ref):
        cols = cols_ref[...]
        hit = lax.broadcasted_iota(jnp.int32, (rows, agg_rows), 1).astype(F32)
        hit = jnp.where(hit == cols[:, 18:19], 1.0, 0.0).astype(BF16)
        hi, lo = halves(up_ref[...])
        picked = nn(hit, hi) + nn(hit, lo)
        part = lax.broadcasted_iota(jnp.int32, (rows, width), 1) // cb
        picked = jnp.where(part.astype(F32) == cols[:, 19:20], picked, 0.0)
        out_ref[...] = x_ref[...] + times(picked, (rh_ref[...], rl_ref[...]), nn)

    (corrected,) = call(correct, [block], update.reshape(agg_rows, width), field, cols, rh, rl)
    return corrected.reshape(right_side.shape), residual.reshape(right_side.shape)


def solution(mesh):
    in_specs = (
        P("line", "tx", "ty", None),
        P("line", "tx", "ty", None),
        P("line", "tx", "ty", None, None),
        P("line", "tx", "ty"),
        P("line", "tx", "ty"),
        P(),
        P(),
        P(),
        P(None, "line", "tx", "ty"),
        P(None, "line", "tx", "ty"),
        P("line", "tx", "ty"),
        P(),
        P("line", "tx", "ty", None, None),
    )
    out_specs = (P("line", "tx", "ty", None), P("line", "tx", "ty", None))
    return jax.shard_map(body, mesh=mesh, in_specs=in_specs, out_specs=out_specs, check_vma=False)
```

```python
import functools

import jax
import jax.numpy as jnp
from jax import lax
from jax.experimental import pallas as pl
from jax.experimental.pallas import tpu as pltpu
from jax.sharding import PartitionSpec as P

SWEEPS = 2
F32 = jnp.float32
BF16 = jnp.bfloat16
SPEC = pl.BlockSpec(memory_space=pltpu.VMEM)


def call(kernel, outs, *args, scratch=(), whole=0):
    return pl.pallas_call(
        kernel,
        in_specs=[pl.BlockSpec(memory_space=pltpu.HBM)] * whole + [SPEC] * (len(args) - whole),
        out_specs=[SPEC] * len(outs),
        out_shape=[pltpu.VMEM(s, d) for s, d in outs],
        scratch_shapes=list(scratch),
        compiler_params=pltpu.CompilerParams(vmem_limit_bytes=24 << 20),
    )(
        *[pltpu.with_memory_space_constraint(a, pltpu.HBM) for a in args[:whole]],
        *[pltpu.with_memory_space_constraint(a, pltpu.VMEM) for a in args[whole:]],
    )


def halves(v):
    hi = v.astype(BF16)
    return hi, (v - hi.astype(F32)).astype(BF16)


def nt(a, b):
    return lax.dot_general(a, b, (((1,), (1,)), ((), ())), preferred_element_type=F32)


def nn(a, b):
    return lax.dot_general(a, b, (((1,), (0,)), ((), ())), preferred_element_type=F32)


def times(v, m, dot=nt):
    n = v.shape[0]
    hi, lo = halves(v)
    both = dot(jnp.concatenate([hi, lo], 0), m[0])
    return both[:n] + both[n:] + dot(hi, m[1])


def each_line(v, weights, lines):
    hi, lo = halves(v)
    out = nt(jnp.concatenate([hi, lo], 0), weights)
    row = lax.broadcasted_iota(jnp.int32, (2 * lines, 128), 0)
    row = jnp.where(row >= lines, row - lines, row)
    acc = jnp.zeros((2 * lines, 128), F32)
    for l in range(lines):
        acc = acc + jnp.where(row == l, out[:, l * 128 : (l + 1) * 128], 0.0)
    return acc[:lines] + acc[lines:]


def forward(g, inc, w_ref, low, cols, n, lines):
    carry, ys = inc, []
    for i in range(n):
        at = slice(i * lines, (i + 1) * lines)
        inner = g[at] - cols[at, 16:17] * times(carry, low)
        carry = each_line(inner, w_ref[i * lines * 128 : (i + 1) * lines * 128, :], lines)
        ys.append(carry)
    return ys


def backward(y, arr, w_ref, upp, cols, n, lines):
    carry, xs = arr, [None] * n
    for i in reversed(range(n)):
        at = slice(i * lines, (i + 1) * lines)
        inner = cols[at, 17:18] * times(carry, upp)
        carry = y[at] - each_line(inner, w_ref[i * lines * 128 : (i + 1) * lines * 128, :], lines)
        xs[i] = carry
    return xs


def is_even(axis):
    return lax.axis_index(axis) % 2 == 0


def put_edges(x_ref, outs, n, lx, ly):
    a_ref, b_ref, c_ref, d_ref = outs
    lines = lx * ly
    first = jnp.concatenate([x_ref[i * lines : i * lines + ly, :] for i in range(n)], 0)
    last = jnp.concatenate([x_ref[(i + 1) * lines - ly : (i + 1) * lines, :] for i in range(n)], 0)
    even = is_even("tx")
    a_ref[...] = jnp.where(even, last, first)
    b_ref[...] = jnp.where(even, first, last)
    first = x_ref[pl.ds(0, n * lx, stride=ly), :]
    last = x_ref[pl.ds(ly - 1, n * lx, stride=ly), :]
    even = is_even("ty")
    c_ref[...] = jnp.where(even, last, first)
    d_ref[...] = jnp.where(even, first, last)


def tangential(x_ref, got, cols, blocks, near, n, lx, ly):
    lines = lx * ly
    x = x_ref[...]
    even = is_even("tx")
    b, c, d, a = (r[...] for r in got)
    below, above = jnp.where(even, b, a), jnp.where(even, a, b)
    near[0] = pltpu.roll(x, ly, 0)
    near[1] = pltpu.roll(x, n * lines - ly, 0)
    for i in range(n):
        near[0, i * lines : i * lines + ly, :] = below[i * ly : (i + 1) * ly]
        near[1, (i + 1) * lines - ly : (i + 1) * lines, :] = above[i * ly : (i + 1) * ly]
    even = is_even("ty")
    below, above = jnp.where(even, d, c), jnp.where(even, c, d)
    row = lax.broadcasted_iota(jnp.int32, x.shape, 0) % ly
    near[2] = pltpu.roll(x, 1, 0)
    near[3] = pltpu.roll(x, n * lines - 1, 0)
    for q in range(n * lx):
        near[2, q * ly : q * ly + 1, :] = below[q : q + 1]
        near[3, q * ly + ly - 1 : q * ly + ly, :] = above[q : q + 1]
    total = jnp.zeros(x.shape, F32)
    beside = [near[s] for s in range(4)]
    for k in range(4):
        mixed = sum(cols[:, 4 * s + k : 4 * s + k + 1] * beside[s] for s in range(4))
        total = total + times(mixed, (blocks[0][k], blocks[1][k]))
    return total


def each_line_pair(v, high, low, lines):
    hi, lo = halves(v)
    both = nt(jnp.concatenate([hi, lo], 0), high)
    out = both[:lines] + both[lines:] + nt(hi, low)
    row = lax.broadcasted_iota(jnp.int32, (lines, 128), 0)
    acc = jnp.zeros((lines, 128), F32)
    for l in range(lines):
        acc = acc + jnp.where(row == l, out[:, l * 128 : (l + 1) * 128], 0.0)
    return acc


def advance(prev, out, mat, w_ref, cols_ref, col, i, lines, base=None):
    group = lines // 2
    left = jnp.concatenate([mat[0], mat[0], mat[1]], 1)

    def some(t, _):
        for j in range(group):
            l = t * group + j
            if prev is None:
                xh, xl = mat
            else:
                hi, lo = halves(prev[l])
                xh, xl = halves(nn(left, jnp.concatenate([hi, lo, hi], 0)))
            at = i * lines + l
            w = w_ref[pl.ds(pl.multiple_of(at * 128, 128), 128), :]
            y = nn(jnp.concatenate([w, w], 1), jnp.concatenate([xh, xl], 0))
            y = y * cols_ref[pl.ds(at, 1), col : col + 1]
            out[l] = -y if base is None else base[l] - y
        return 0

    lax.fori_loop(0, lines // group, some, 0)


def put_halves(src, high, low, lines):
    def one(l, _):
        at = pl.ds(pl.multiple_of(l * 128, 128), 128)
        high[at, :], low[at, :] = halves(src[l])
        return 0

    lax.fori_loop(0, lines, one, 0)


def swaps(count, start):
    return [
        pair
        for i in range(start, count - 1, 2)
        for pair in ((i, i + 1), (i + 1, i))
    ]


def exchange(sends):
    nx, ny = lax.axis_size("tx"), lax.axis_size("ty")
    a, b, c, d = sends
    d = lax.ppermute(d, "ty", swaps(ny, 1))
    c = lax.ppermute(c, "ty", swaps(ny, 0))
    b = lax.ppermute(b, "tx", swaps(nx, 1))
    a = lax.ppermute(a, "tx", swaps(nx, 0))
    return b, c, d, a


def body(
    right_side,
    start_field,
    line_inverse,
    lower_scale,
    upper_scale,
    lower_block,
    upper_block,
    face_blocks,
    face_kind,
    face_scale,
    agglomerate,
    restriction,
    coarse_inverse,
):
    n, lx, ly, width = right_side.shape
    lines, rows, cb = lx * ly, n * lx * ly, restriction.shape[0]
    quarter = width // cb
    segments, owners = lax.axis_size("line"), lax.axis_size("ty")
    owned_rows = coarse_inverse.shape[2] // quarter
    agg_rows = owned_rows * owners
    rhs = right_side.reshape(rows, width)
    start = start_field.reshape(rows, width)
    w = line_inverse.reshape(rows * width, width)

    block, edge = ((rows, width), F32), ((lines, width), F32)
    half, half4 = ((width, width), BF16), ((4, width, width), BF16)
    edges4 = [((n * ly, width), F32)] * 2 + [((n * lx, width), F32)] * 2

    def first_edges(x_ref, *outs):
        put_edges(x_ref, outs, n, lx, ly)

    sends = call(first_edges, edges4, start)

    raw = (
        w,
        lower_block,
        upper_block,
        face_blocks,
        restriction,
        coarse_inverse.reshape(owned_rows * width, cb),
        face_kind,
        face_scale,
        lower_scale,
        upper_scale,
        agglomerate,
    )

    def prepare(*refs):
        outs = refs[len(raw) : len(raw) + 13]
        held, sems = refs[len(raw) + 13 : -1], refs[-1]
        copies = [
            pltpu.make_async_copy(src, dst, sems.at[k])
            for k, (src, dst) in enumerate(zip(refs, (outs[10], *held)))
        ]
        for copy in copies:
            copy.start()
        for copy in copies[1:]:
            copy.wait()
        l_ref, u_ref, f_ref, r_ref, c_ref, kind_ref, face_ref, low_ref, up_ref, agg_ref = held
        for k, src in enumerate((l_ref, u_ref, f_ref)):
            outs[2 * k][...], outs[2 * k + 1][...] = halves(src[...])
        outs[6][...], outs[7][...] = halves(jnp.concatenate([r_ref[...]] * quarter, 0))
        lane = lax.broadcasted_iota(jnp.int32, (cb, width), 1) % cb
        wide = (lane == lax.broadcasted_iota(jnp.int32, (cb, width), 0)).astype(F32).astype(BF16)
        part = (lax.broadcasted_iota(jnp.int32, (owned_rows * width, width), 0) // cb) % quarter
        mine = part == lax.broadcasted_iota(jnp.int32, (owned_rows * width, width), 1) // cb
        for k, piece in enumerate(halves(c_ref[...])):
            outs[8 + k][...] = jnp.where(mine, nn(piece, wide), 0.0).astype(BF16)
        groups = rows // ly
        row = lax.broadcasted_iota(jnp.int32, (rows, groups), 0)
        up = (row // ly == lax.broadcasted_iota(jnp.int32, (rows, groups), 1)).astype(F32).astype(BF16)
        row = lax.broadcasted_iota(jnp.int32, (rows, ly), 0)
        own = row % ly == lax.broadcasted_iota(jnp.int32, (rows, ly), 1)

        def column(ref, *at):
            src = jnp.concatenate([ref[(*at, i)] for i in range(n)], 0).astype(F32)
            hi, lo = halves(src)
            return jnp.sum(jnp.where(own, nn(up, hi) + nn(up, lo), 0.0), axis=1, keepdims=True)

        agg = column(agg_ref).astype(jnp.int32)
        row_of = (agg // quarter).astype(F32)
        listed = []
        for side in range(4):
            kind, face = column(kind_ref, side), column(face_ref, side)
            listed += [jnp.where(kind == float(k), face, 0.0) for k in range(4)]
        listed += [column(low_ref), column(up_ref), row_of, (agg % quarter).astype(F32)]
        lane = lax.broadcasted_iota(jnp.int32, (rows, width), 1)
        cols = jnp.zeros((rows, width), F32)
        for k, value in enumerate(listed):
            cols = jnp.where(lane == k, value, cols)
        outs[11][...] = cols
        square = lax.broadcasted_iota(jnp.int32, (rows, rows), 0) == lax.broadcasted_iota(jnp.int32, (rows, rows), 1)
        across = jnp.sum(jnp.where(square, row_of, 0.0), axis=0, keepdims=True)
        outs[12][...] = jnp.broadcast_to(across, (8, rows))
        copies[0].wait()

    lh, ll, uh, ul, fh, fl, rh, rl, ch, cl, w, cols, agg_lane = call(
        prepare,
        [half, half, half, half, half4, half4, half, half]
        + [((owned_rows * width, width), BF16)] * 2
        + [((rows * width, width), BF16), block, ((8, rows), F32)],
        *raw,
        scratch=[pltpu.VMEM(a.shape, a.dtype) for a in raw[1:]]
        + [pltpu.SemaphoreType.DMA((len(raw),))],
        whole=len(raw),
    )

    def open_forward(x_ref, a, b, c, d, cols_ref, fh_ref, fl_ref, rhs_ref, lh_ref, ll_ref, w_ref, g_ref, y_ref, f_ref, near):
        cols = cols_ref[...]
        total = tangential(x_ref, (a, b, c, d), cols, (fh_ref, fl_ref), near, n, lx, ly)
        g = rhs_ref[...] - total
        g_ref[...] = g
        zero = jnp.zeros((lines, width), F32)
        ys = forward(g, zero, w_ref, (lh_ref[...], ll_ref[...]), cols, n, lines)
        y_ref[...] = jnp.concatenate(ys, 0)
        f_ref[...] = ys[-1]

    def backward_map(after_ref, cols_ref, uh_ref, ul_ref, w_ref, high, low, one, two):
        pos = lax.axis_index("line")

        @pl.when((pos > 0) & (pos < segments - 1))
        def _():
            mat, prev = (uh_ref[...], ul_ref[...]), None
            for i in reversed(range(n)):
                now = (one, two)[i % 2]
                advance(prev, now, mat, w_ref, cols_ref, 17, i, lines)
                prev = now
            put_halves(prev, high, low, lines)

    def turn_map(after_ref, cols_ref, lh_ref, ll_ref, uh_ref, ul_ref, w_ref, high, low, steps, one, two):
        @pl.when(lax.axis_index("line") == segments - 1)
        def _():
            mat, prev = (lh_ref[...], ll_ref[...]), None
            for i in range(n):
                advance(prev, steps.at[i], mat, w_ref, cols_ref, 16, i, lines)
                prev = steps.at[i]
            mat = (uh_ref[...], ul_ref[...])
            for i in reversed(range(n - 1)):
                now = (one, two)[i % 2]
                advance(prev, now, mat, w_ref, cols_ref, 17, i, lines, steps.at[i])
                prev = now
            put_halves(prev, high, low, lines)

    def chain_forward(stage, g_ref, inc_ref, got_ref, cols_ref, lh_ref, ll_ref, w_ref, sum_ref, f_ref):
        inc = inc_ref[...] + got_ref[...]
        sum_ref[...] = inc

        @pl.when(lax.axis_index("line") == stage)
        def _():
            ys = forward(g_ref[...], inc, w_ref, (lh_ref[...], ll_ref[...]), cols_ref[...], n, lines)
            f_ref[...] = ys[-1]

    def chain_turn(g_ref, inc_ref, got_ref, cols_ref, lh_ref, ll_ref, uh_ref, ul_ref, w_ref, y_ref, x_ref):
        cols = cols_ref[...]
        inc = inc_ref[...] + got_ref[...]
        ys = forward(g_ref[...], inc, w_ref, (lh_ref[...], ll_ref[...]), cols, n, lines)
        for i in range(n):
            y_ref[i * lines : (i + 1) * lines, :] = ys[i]

        @pl.when(lax.axis_index("line") == segments - 1)
        def _():
            zero = jnp.zeros((lines, width), F32)
            x_ref[...] = backward(y_ref[...], zero, w_ref, (uh_ref[...], ul_ref[...]), cols, n, lines)[0]

    def chain_backward(stage, y_ref, arr_ref, got_ref, cols_ref, uh_ref, ul_ref, w_ref, after, after_too, sum_ref, x_ref):
        arr = arr_ref[...] + got_ref[...]
        sum_ref[...] = arr

        @pl.when(lax.axis_index("line") == stage)
        def _():
            xs = backward(y_ref[...], arr, w_ref, (uh_ref[...], ul_ref[...]), cols_ref[...], n, lines)
            x_ref[...] = xs[0]

    def local_back(after_ref, y_ref, cols_ref, uh_ref, ul_ref, w_ref, x_ref):
        zero = jnp.zeros((lines, width), F32)
        x_ref[...] = backward(y_ref[...], zero, w_ref, (uh_ref[...], ul_ref[...]), cols_ref[...], n, lines)[0]

    def turn(local_ref, inc_ref, got_ref, high, low, sum_ref, x_ref):
        inc = inc_ref[...] + got_ref[...]
        sum_ref[...] = inc
        x_ref[...] = local_ref[...] + each_line_pair(inc, high[...], low[...], lines)

    def settle(after_ref, g_ref, inc_ref, cols_ref, lh_ref, ll_ref, uh_ref, ul_ref, w_ref, y_ref, x_ref):
        cols = cols_ref[...]
        ys = forward(g_ref[...], inc_ref[...], w_ref, (lh_ref[...], ll_ref[...]), cols, n, lines)
        y = jnp.concatenate(ys, 0)
        y_ref[...] = y
        zero = jnp.zeros((lines, width), F32)
        x_ref[...] = backward(y, zero, w_ref, (uh_ref[...], ul_ref[...]), cols, n, lines)[0]

    def next_backward(first_ref, arr_ref, got_ref, high, low, sum_ref, x_ref):
        arr = arr_ref[...] + got_ref[...]
        sum_ref[...] = arr
        x_ref[...] = first_ref[...] + each_line_pair(arr, high[...], low[...], lines)

    def close_backward(last, y_ref, arr_ref, got_ref, prev_ref, cols_ref, uh_ref, ul_ref, w_ref, x_ref, d_ref, *outs):
        arr = arr_ref[...] + got_ref[...]
        xs = backward(y_ref[...], arr, w_ref, (uh_ref[...], ul_ref[...]), cols_ref[...], n, lines)
        x = jnp.concatenate(xs, 0)
        x_ref[...] = x
        d_ref[...] = prev_ref[...] - x
        put_edges(d_ref if last else x_ref, outs, n, lx, ly)

    pair = [((lines * width, width), BF16)] * 2
    two = [pltpu.VMEM((lines, width, width), F32)] * 2
    field = start
    change = None
    for sweep in range(SWEEPS):
        got = exchange(sends)
        g, y, ahead = call(
            open_forward,
            [block, block, edge],
            field, *got, cols, fh, fl, rhs, lh, ll, w,
            scratch=[pltpu.VMEM((4, rows, width), F32)],
        )
        inc = arr = jnp.zeros((lines, width), F32)
        if sweep == 0:
            for k in range(segments - 2):
                recv = lax.ppermute(ahead, "line", [(k, k + 1)])
                step = functools.partial(chain_forward, k + 1)
                inc, ahead = call(step, [edge, edge], g, inc, recv, cols, lh, ll, w)
            recv = lax.ppermute(ahead, "line", [(segments - 2, segments - 1)])
            y, behind = call(chain_turn, [block, edge], g, inc, recv, cols, lh, ll, uh, ul, w)
            for k in range(segments - 2):
                recv = lax.ppermute(behind, "line", [(segments - 1 - k, segments - 2 - k)])
                if k == 0:
                    steps = [pltpu.VMEM((n, lines, width, width), F32)]
                    bend = call(turn_map, pair, behind, cols, lh, ll, uh, ul, w, scratch=steps + two)
                if k == segments - 3:
                    back = call(backward_map, pair, behind, cols, uh, ul, w, scratch=two)
                step = functools.partial(chain_backward, segments - 2 - k)
                made = back if k == segments - 3 else bend
                arr, behind = call(step, [edge, edge], y, arr, recv, cols, uh, ul, w, *made)
        else:
            for k in range(segments - 2):
                recv = lax.ppermute(ahead, "line", [(k, k + 1)])
                step = functools.partial(chain_forward, k + 1)
                inc, ahead = call(step, [edge, edge], g, inc, recv, cols, lh, ll, w)
                if k == 0:
                    local = call(local_back, [edge], ahead, y, cols, uh, ul, w)[0]
            recv = lax.ppermute(ahead, "line", [(segments - 2, segments - 1)])
            inc, behind = call(turn, [edge, edge], local, inc, recv, *bend)
            for k in range(segments - 2):
                recv = lax.ppermute(behind, "line", [(segments - 1 - k, segments - 2 - k)])
                if k == 0:
                    y, first = call(settle, [block, edge], behind, g, inc, cols, lh, ll, uh, ul, w)
                arr, behind = call(next_backward, [edge, edge], first, arr, recv, *back)
        recv = lax.ppermute(behind, "line", [(1, 0)])
        out = call(
            functools.partial(close_backward, sweep == SWEEPS - 1),
            [block, block] + edges4,
            y, arr, recv, field, cols, uh, ul, w,
        )
        field, change, sends = out[0], out[1], out[2:]

    got = exchange(sends)

    def restrict(x_ref, a, b, c, d, cols_ref, fh_ref, fl_ref, rh_ref, rl_ref, lane_ref, res_ref, part_ref, near):
        cols = cols_ref[...]
        res = tangential(x_ref, (a, b, c, d), cols, (fh_ref, fl_ref), near, n, lx, ly)
        res_ref[...] = res
        proj = times(res, (rh_ref[...], rl_ref[...]))
        part = lax.broadcasted_iota(jnp.int32, (rows, width), 1) // cb
        proj = jnp.where(part.astype(F32) == cols[:, 19:20], proj, 0.0)
        hit = lax.broadcasted_iota(jnp.int32, (agg_rows, rows), 0).astype(F32)
        hit = jnp.where(hit == lane_ref[0:1, :], 1.0, 0.0).astype(BF16)
        hi, lo = halves(proj)
        part_ref[...] = nn(hit, hi) + nn(hit, lo)

    residual, partial = call(
        restrict,
        [block, ((agg_rows, width), F32)],
        change, *got, cols, fh, fl, rh, rl, agg_lane,
        scratch=[pltpu.VMEM((4, rows, width), F32)],
    )
    parts = lax.all_to_all(partial.reshape(owners, owned_rows, width), "ty", 0, 0, tiled=True)

    def solve_coarse(parts_ref, ch_ref, cl_ref, up_ref):
        sums = parts_ref[0]
        for k in range(1, owners):
            sums = sums + parts_ref[k]
        hi, lo = halves(sums)
        zero = jnp.zeros((8 - owned_rows, width), BF16)
        hi, lo = jnp.concatenate([hi, zero], 0), jnp.concatenate([lo, zero], 0)
        both = jnp.concatenate([hi, lo], 0)
        out = nt(both, ch_ref[...])
        out = out[:8] + out[8:] + nt(both, cl_ref[...])[:8]
        row = lax.broadcasted_iota(jnp.int32, (8, width), 0)
        acc = jnp.zeros((8, width), F32)
        for k in range(owned_rows):
            acc = acc + jnp.where(row == k, out[:, k * width : (k + 1) * width], 0.0)
        for k in range(owners):
            up_ref[k] = acc[:owned_rows]

    (copies,) = call(solve_coarse, [((owners, owned_rows, width), F32)], parts, ch, cl)
    update = lax.all_to_all(copies, "ty", 0, 0, tiled=True)

    def correct(up_ref, x_ref, cols_ref, rh_ref, rl_ref, out_ref):
        cols = cols_ref[...]
        hit = lax.broadcasted_iota(jnp.int32, (rows, agg_rows), 1).astype(F32)
        hit = jnp.where(hit == cols[:, 18:19], 1.0, 0.0).astype(BF16)
        hi, lo = halves(up_ref[...])
        picked = nn(hit, hi) + nn(hit, lo)
        part = lax.broadcasted_iota(jnp.int32, (rows, width), 1) // cb
        picked = jnp.where(part.astype(F32) == cols[:, 19:20], picked, 0.0)
        out_ref[...] = x_ref[...] + times(picked, (rh_ref[...], rl_ref[...]), nn)

    (corrected,) = call(correct, [block], update.reshape(agg_rows, width), field, cols, rh, rl)
    return corrected.reshape(right_side.shape), residual.reshape(right_side.shape)


def solution(mesh):
    in_specs = (
        P("line", "tx", "ty", None),
        P("line", "tx", "ty", None),
        P("line", "tx", "ty", None, None),
        P("line", "tx", "ty"),
        P("line", "tx", "ty"),
        P(),
        P(),
        P(),
        P(None, "line", "tx", "ty"),
        P(None, "line", "tx", "ty"),
        P("line", "tx", "ty"),
        P(),
        P("line", "tx", "ty", None, None),
    )
    out_specs = (P("line", "tx", "ty", None), P("line", "tx", "ty", None))
    return jax.shard_map(body, mesh=mesh, in_specs=in_specs, out_specs=out_specs, check_vma=False)
```

```python
import functools

import jax
import jax.numpy as jnp
from jax import lax
from jax.experimental import pallas as pl
from jax.experimental.pallas import tpu as pltpu
from jax.sharding import PartitionSpec as P

SWEEPS = 2
F32 = jnp.float32
BF16 = jnp.bfloat16
SPEC = pl.BlockSpec(memory_space=pltpu.VMEM)


def call(kernel, outs, *args, scratch=(), whole=0):
    return pl.pallas_call(
        kernel,
        in_specs=[pl.BlockSpec(memory_space=pltpu.HBM)] * whole + [SPEC] * (len(args) - whole),
        out_specs=[SPEC] * len(outs),
        out_shape=[pltpu.VMEM(s, d) for s, d in outs],
        scratch_shapes=list(scratch),
        compiler_params=pltpu.CompilerParams(vmem_limit_bytes=24 << 20),
    )(
        *[pltpu.with_memory_space_constraint(a, pltpu.HBM) for a in args[:whole]],
        *[pltpu.with_memory_space_constraint(a, pltpu.VMEM) for a in args[whole:]],
    )


def halves(v):
    hi = v.astype(BF16)
    return hi, (v - hi.astype(F32)).astype(BF16)


def nt(a, b):
    return lax.dot_general(a, b, (((1,), (1,)), ((), ())), preferred_element_type=F32)


def nn(a, b):
    return lax.dot_general(a, b, (((1,), (0,)), ((), ())), preferred_element_type=F32)


def times(v, m, dot=nt):
    n = v.shape[0]
    hi, lo = halves(v)
    both = dot(jnp.concatenate([hi, lo], 0), m[0])
    return both[:n] + both[n:] + dot(hi, m[1])


def each_line(v, weights, lines):
    hi, lo = halves(v)
    out = nt(jnp.concatenate([hi, lo], 0), weights)
    row = lax.broadcasted_iota(jnp.int32, (2 * lines, 128), 0)
    row = jnp.where(row >= lines, row - lines, row)
    acc = jnp.zeros((2 * lines, 128), F32)
    for l in range(lines):
        acc = acc + jnp.where(row == l, out[:, l * 128 : (l + 1) * 128], 0.0)
    return acc[:lines] + acc[lines:]


def forward(g, inc, w_ref, low, cols, n, lines):
    carry, ys = inc, []
    for i in range(n):
        at = slice(i * lines, (i + 1) * lines)
        inner = g[at] - cols[at, 16:17] * times(carry, low)
        carry = each_line(inner, w_ref[i * lines * 128 : (i + 1) * lines * 128, :], lines)
        ys.append(carry)
    return ys


def backward(y, arr, w_ref, upp, cols, n, lines):
    carry, xs = arr, [None] * n
    for i in reversed(range(n)):
        at = slice(i * lines, (i + 1) * lines)
        inner = cols[at, 17:18] * times(carry, upp)
        carry = y[at] - each_line(inner, w_ref[i * lines * 128 : (i + 1) * lines * 128, :], lines)
        xs[i] = carry
    return xs


def is_even(axis):
    return lax.axis_index(axis) % 2 == 0


def put_edges(x_ref, outs, n, lx, ly):
    a_ref, b_ref, c_ref, d_ref = outs
    lines = lx * ly
    first = jnp.concatenate([x_ref[i * lines : i * lines + ly, :] for i in range(n)], 0)
    last = jnp.concatenate([x_ref[(i + 1) * lines - ly : (i + 1) * lines, :] for i in range(n)], 0)
    even = is_even("tx")
    a_ref[...] = jnp.where(even, last, first)
    b_ref[...] = jnp.where(even, first, last)
    first = x_ref[pl.ds(0, n * lx, stride=ly), :]
    last = x_ref[pl.ds(ly - 1, n * lx, stride=ly), :]
    even = is_even("ty")
    c_ref[...] = jnp.where(even, last, first)
    d_ref[...] = jnp.where(even, first, last)


def tangential(x_ref, got, cols, blocks, near, n, lx, ly):
    lines = lx * ly
    x = x_ref[...]
    even = is_even("tx")
    b, c, d, a = (r[...] for r in got)
    below, above = jnp.where(even, b, a), jnp.where(even, a, b)
    near[0] = pltpu.roll(x, ly, 0)
    near[1] = pltpu.roll(x, n * lines - ly, 0)
    for i in range(n):
        near[0, i * lines : i * lines + ly, :] = below[i * ly : (i + 1) * ly]
        near[1, (i + 1) * lines - ly : (i + 1) * lines, :] = above[i * ly : (i + 1) * ly]
    even = is_even("ty")
    below, above = jnp.where(even, d, c), jnp.where(even, c, d)
    row = lax.broadcasted_iota(jnp.int32, x.shape, 0) % ly
    near[2] = pltpu.roll(x, 1, 0)
    near[3] = pltpu.roll(x, n * lines - 1, 0)
    for q in range(n * lx):
        near[2, q * ly : q * ly + 1, :] = below[q : q + 1]
        near[3, q * ly + ly - 1 : q * ly + ly, :] = above[q : q + 1]
    total = jnp.zeros(x.shape, F32)
    beside = [near[s] for s in range(4)]
    for k in range(4):
        mixed = sum(cols[:, 4 * s + k : 4 * s + k + 1] * beside[s] for s in range(4))
        total = total + times(mixed, (blocks[0][k], blocks[1][k]))
    return total


def each_line_pair(v, high, low, lines):
    hi, lo = halves(v)
    both = nt(jnp.concatenate([hi, lo], 0), high)
    out = both[:lines] + both[lines:] + nt(hi, low)
    row = lax.broadcasted_iota(jnp.int32, (lines, 128), 0)
    acc = jnp.zeros((lines, 128), F32)
    for l in range(lines):
        acc = acc + jnp.where(row == l, out[:, l * 128 : (l + 1) * 128], 0.0)
    return acc


def advance(prev, out, mat, w_ref, cols_ref, col, i, lines, base=None):
    group = lines // 2
    left = jnp.concatenate([mat[0], mat[0], mat[1]], 1)

    def some(t, _):
        for j in range(group):
            l = t * group + j
            if prev is None:
                xh, xl = mat
            else:
                hi, lo = halves(prev[l])
                xh, xl = halves(nn(left, jnp.concatenate([hi, lo, hi], 0)))
            at = i * lines + l
            w = w_ref[pl.ds(pl.multiple_of(at * 128, 128), 128), :]
            y = nn(jnp.concatenate([w, w], 1), jnp.concatenate([xh, xl], 0))
            y = y * cols_ref[pl.ds(at, 1), col : col + 1]
            out[l] = -y if base is None else base[l] - y
        return 0

    lax.fori_loop(0, lines // group, some, 0)


def put_halves(src, high, low, lines):
    def one(l, _):
        at = pl.ds(pl.multiple_of(l * 128, 128), 128)
        high[at, :], low[at, :] = halves(src[l])
        return 0

    lax.fori_loop(0, lines, one, 0)


def swaps(count, start):
    return [
        pair
        for i in range(start, count - 1, 2)
        for pair in ((i, i + 1), (i + 1, i))
    ]


def exchange(sends):
    nx, ny = lax.axis_size("tx"), lax.axis_size("ty")
    a, b, c, d = sends
    d = lax.ppermute(d, "ty", swaps(ny, 1))
    c = lax.ppermute(c, "ty", swaps(ny, 0))
    b = lax.ppermute(b, "tx", swaps(nx, 1))
    a = lax.ppermute(a, "tx", swaps(nx, 0))
    return b, c, d, a


def body(
    right_side,
    start_field,
    line_inverse,
    lower_scale,
    upper_scale,
    lower_block,
    upper_block,
    face_blocks,
    face_kind,
    face_scale,
    agglomerate,
    restriction,
    coarse_inverse,
):
    n, lx, ly, width = right_side.shape
    lines, rows, cb = lx * ly, n * lx * ly, restriction.shape[0]
    quarter = width // cb
    segments, owners = lax.axis_size("line"), lax.axis_size("ty")
    owned_rows = coarse_inverse.shape[2] // quarter
    agg_rows = owned_rows * owners
    rhs = right_side.reshape(rows, width)
    start = start_field.reshape(rows, width)
    w = line_inverse.reshape(rows * width, width)

    block, edge = ((rows, width), F32), ((lines, width), F32)
    half, half4 = ((width, width), BF16), ((4, width, width), BF16)
    edges4 = [((n * ly, width), F32)] * 2 + [((n * lx, width), F32)] * 2

    def first_edges(x_ref, *outs):
        put_edges(x_ref, outs, n, lx, ly)

    sends = call(first_edges, edges4, start)

    raw = (
        w,
        lower_block,
        upper_block,
        face_blocks,
        restriction,
        coarse_inverse.reshape(owned_rows * width, cb),
        face_kind,
        face_scale,
        lower_scale,
        upper_scale,
        agglomerate,
    )

    def prepare(*refs):
        outs = refs[len(raw) : len(raw) + 13]
        held, sems = refs[len(raw) + 13 : -1], refs[-1]
        copies = [
            pltpu.make_async_copy(src, dst, sems.at[k])
            for k, (src, dst) in enumerate(zip(refs, (outs[10], *held)))
        ]
        for copy in copies:
            copy.start()
        for copy in copies[1:]:
            copy.wait()
        l_ref, u_ref, f_ref, r_ref, c_ref, kind_ref, face_ref, low_ref, up_ref, agg_ref = held
        for k, src in enumerate((l_ref, u_ref, f_ref)):
            outs[2 * k][...], outs[2 * k + 1][...] = halves(src[...])
        outs[6][...], outs[7][...] = halves(jnp.concatenate([r_ref[...]] * quarter, 0))
        lane = lax.broadcasted_iota(jnp.int32, (cb, width), 1) % cb
        wide = (lane == lax.broadcasted_iota(jnp.int32, (cb, width), 0)).astype(F32).astype(BF16)
        part = (lax.broadcasted_iota(jnp.int32, (owned_rows * width, width), 0) // cb) % quarter
        mine = part == lax.broadcasted_iota(jnp.int32, (owned_rows * width, width), 1) // cb
        for k, piece in enumerate(halves(c_ref[...])):
            outs[8 + k][...] = jnp.where(mine, nn(piece, wide), 0.0).astype(BF16)
        groups = rows // ly
        row = lax.broadcasted_iota(jnp.int32, (rows, groups), 0)
        up = (row // ly == lax.broadcasted_iota(jnp.int32, (rows, groups), 1)).astype(F32).astype(BF16)
        row = lax.broadcasted_iota(jnp.int32, (rows, ly), 0)
        own = row % ly == lax.broadcasted_iota(jnp.int32, (rows, ly), 1)

        def column(ref, *at):
            src = jnp.concatenate([ref[(*at, i)] for i in range(n)], 0).astype(F32)
            hi, lo = halves(src)
            return jnp.sum(jnp.where(own, nn(up, hi) + nn(up, lo), 0.0), axis=1, keepdims=True)

        agg = column(agg_ref).astype(jnp.int32)
        row_of = (agg // quarter).astype(F32)
        listed = []
        for side in range(4):
            kind, face = column(kind_ref, side), column(face_ref, side)
            listed += [jnp.where(kind == float(k), face, 0.0) for k in range(4)]
        listed += [column(low_ref), column(up_ref), row_of, (agg % quarter).astype(F32)]
        lane = lax.broadcasted_iota(jnp.int32, (rows, width), 1)
        cols = jnp.zeros((rows, width), F32)
        for k, value in enumerate(listed):
            cols = jnp.where(lane == k, value, cols)
        outs[11][...] = cols
        square = lax.broadcasted_iota(jnp.int32, (rows, rows), 0) == lax.broadcasted_iota(jnp.int32, (rows, rows), 1)
        across = jnp.sum(jnp.where(square, row_of, 0.0), axis=0, keepdims=True)
        outs[12][...] = jnp.broadcast_to(across, (8, rows))
        copies[0].wait()

    lh, ll, uh, ul, fh, fl, rh, rl, ch, cl, w, cols, agg_lane = call(
        prepare,
        [half, half, half, half, half4, half4, half, half]
        + [((owned_rows * width, width), BF16)] * 2
        + [((rows * width, width), BF16), block, ((8, rows), F32)],
        *raw,
        scratch=[pltpu.VMEM(a.shape, a.dtype) for a in raw[1:]]
        + [pltpu.SemaphoreType.DMA((len(raw),))],
        whole=len(raw),
    )

    def open_forward(x_ref, a, b, c, d, cols_ref, fh_ref, fl_ref, rhs_ref, lh_ref, ll_ref, w_ref, g_ref, f_ref, near):
        cols = cols_ref[...]
        total = tangential(x_ref, (a, b, c, d), cols, (fh_ref, fl_ref), near, n, lx, ly)
        g = rhs_ref[...] - total
        g_ref[...] = g

        @pl.when(lax.axis_index("line") == 0)
        def _():
            zero = jnp.zeros((lines, width), F32)
            f_ref[...] = forward(g, zero, w_ref, (lh_ref[...], ll_ref[...]), cols, n, lines)[-1]

    def backward_map(after_ref, cols_ref, uh_ref, ul_ref, w_ref, high, low, one, two):
        pos = lax.axis_index("line")

        @pl.when((pos > 0) & (pos < segments - 1))
        def _():
            mat, prev = (uh_ref[...], ul_ref[...]), None
            for i in reversed(range(n)):
                now = (one, two)[i % 2]
                advance(prev, now, mat, w_ref, cols_ref, 17, i, lines)
                prev = now
            put_halves(prev, high, low, lines)

    def turn_map(after_ref, cols_ref, lh_ref, ll_ref, uh_ref, ul_ref, w_ref, high, low, steps, one, two):
        @pl.when(lax.axis_index("line") == segments - 1)
        def _():
            mat, prev = (lh_ref[...], ll_ref[...]), None
            for i in range(n):
                advance(prev, steps.at[i], mat, w_ref, cols_ref, 16, i, lines)
                prev = steps.at[i]
            mat = (uh_ref[...], ul_ref[...])
            for i in reversed(range(n - 1)):
                now = (one, two)[i % 2]
                advance(prev, now, mat, w_ref, cols_ref, 17, i, lines, steps.at[i])
                prev = now
            put_halves(prev, high, low, lines)

    def chain_forward(stage, g_ref, inc_ref, got_ref, cols_ref, lh_ref, ll_ref, w_ref, sum_ref, f_ref):
        inc = inc_ref[...] + got_ref[...]
        sum_ref[...] = inc

        @pl.when(lax.axis_index("line") == stage)
        def _():
            ys = forward(g_ref[...], inc, w_ref, (lh_ref[...], ll_ref[...]), cols_ref[...], n, lines)
            f_ref[...] = ys[-1]

    def chain_turn(g_ref, inc_ref, got_ref, cols_ref, lh_ref, ll_ref, uh_ref, ul_ref, w_ref, y_ref, x_ref):
        cols = cols_ref[...]
        inc = inc_ref[...] + got_ref[...]
        ys = forward(g_ref[...], inc, w_ref, (lh_ref[...], ll_ref[...]), cols, n, lines)
        for i in range(n):
            y_ref[i * lines : (i + 1) * lines, :] = ys[i]

        @pl.when(lax.axis_index("line") == segments - 1)
        def _():
            zero = jnp.zeros((lines, width), F32)
            x_ref[...] = backward(y_ref[...], zero, w_ref, (uh_ref[...], ul_ref[...]), cols, n, lines)[0]

    def chain_backward(stage, y_ref, arr_ref, got_ref, cols_ref, uh_ref, ul_ref, w_ref, after, after_too, sum_ref, x_ref):
        arr = arr_ref[...] + got_ref[...]
        sum_ref[...] = arr

        @pl.when(lax.axis_index("line") == stage)
        def _():
            xs = backward(y_ref[...], arr, w_ref, (uh_ref[...], ul_ref[...]), cols_ref[...], n, lines)
            x_ref[...] = xs[0]

    def local_back(after_ref, g_ref, cols_ref, lh_ref, ll_ref, uh_ref, ul_ref, w_ref, x_ref):
        cols = cols_ref[...]
        zero = jnp.zeros((lines, width), F32)
        ys = forward(g_ref[...], zero, w_ref, (lh_ref[...], ll_ref[...]), cols, n, lines)
        y = jnp.concatenate(ys, 0)
        x_ref[...] = backward(y, zero, w_ref, (uh_ref[...], ul_ref[...]), cols, n, lines)[0]

    def turn(local_ref, inc_ref, got_ref, high, low, sum_ref, x_ref):
        inc = inc_ref[...] + got_ref[...]
        sum_ref[...] = inc
        x_ref[...] = local_ref[...] + each_line_pair(inc, high[...], low[...], lines)

    def settle(after_ref, g_ref, inc_ref, cols_ref, lh_ref, ll_ref, uh_ref, ul_ref, w_ref, y_ref, x_ref):
        cols = cols_ref[...]
        ys = forward(g_ref[...], inc_ref[...], w_ref, (lh_ref[...], ll_ref[...]), cols, n, lines)
        y = jnp.concatenate(ys, 0)
        y_ref[...] = y
        zero = jnp.zeros((lines, width), F32)
        x_ref[...] = backward(y, zero, w_ref, (uh_ref[...], ul_ref[...]), cols, n, lines)[0]

    def next_backward(first_ref, arr_ref, got_ref, high, low, sum_ref, x_ref):
        arr = arr_ref[...] + got_ref[...]
        sum_ref[...] = arr
        x_ref[...] = first_ref[...] + each_line_pair(arr, high[...], low[...], lines)

    def close_backward(last, y_ref, arr_ref, got_ref, prev_ref, cols_ref, uh_ref, ul_ref, w_ref, x_ref, d_ref, *outs):
        arr = arr_ref[...] + got_ref[...]
        xs = backward(y_ref[...], arr, w_ref, (uh_ref[...], ul_ref[...]), cols_ref[...], n, lines)
        x = jnp.concatenate(xs, 0)
        x_ref[...] = x
        d_ref[...] = prev_ref[...] - x
        put_edges(d_ref if last else x_ref, outs, n, lx, ly)

    pair = [((lines * width, width), BF16)] * 2
    two = [pltpu.VMEM((lines, width, width), F32)] * 2
    field = start
    change = None
    for sweep in range(SWEEPS):
        got = exchange(sends)
        g, ahead = call(
            open_forward,
            [block, edge],
            field, *got, cols, fh, fl, rhs, lh, ll, w,
            scratch=[pltpu.VMEM((4, rows, width), F32)],
        )
        inc = arr = jnp.zeros((lines, width), F32)
        if sweep == 0:
            for k in range(segments - 2):
                recv = lax.ppermute(ahead, "line", [(k, k + 1)])
                step = functools.partial(chain_forward, k + 1)
                inc, ahead = call(step, [edge, edge], g, inc, recv, cols, lh, ll, w)
            recv = lax.ppermute(ahead, "line", [(segments - 2, segments - 1)])
            y, behind = call(chain_turn, [block, edge], g, inc, recv, cols, lh, ll, uh, ul, w)
            for k in range(segments - 2):
                recv = lax.ppermute(behind, "line", [(segments - 1 - k, segments - 2 - k)])
                if k == 0:
                    steps = [pltpu.VMEM((n, lines, width, width), F32)]
                    bend = call(turn_map, pair, behind, cols, lh, ll, uh, ul, w, scratch=steps + two)
                if k == segments - 3:
                    back = call(backward_map, pair, behind, cols, uh, ul, w, scratch=two)
                step = functools.partial(chain_backward, segments - 2 - k)
                made = back if k == segments - 3 else bend
                arr, behind = call(step, [edge, edge], y, arr, recv, cols, uh, ul, w, *made)
        else:
            for k in range(segments - 2):
                recv = lax.ppermute(ahead, "line", [(k, k + 1)])
                step = functools.partial(chain_forward, k + 1)
                inc, ahead = call(step, [edge, edge], g, inc, recv, cols, lh, ll, w)
                if k == 0:
                    local = call(local_back, [edge], ahead, g, cols, lh, ll, uh, ul, w)[0]
            recv = lax.ppermute(ahead, "line", [(segments - 2, segments - 1)])
            inc, behind = call(turn, [edge, edge], local, inc, recv, *bend)
            for k in range(segments - 2):
                recv = lax.ppermute(behind, "line", [(segments - 1 - k, segments - 2 - k)])
                if k == 0:
                    y, first = call(settle, [block, edge], behind, g, inc, cols, lh, ll, uh, ul, w)
                arr, behind = call(next_backward, [edge, edge], first, arr, recv, *back)
        recv = lax.ppermute(behind, "line", [(1, 0)])
        out = call(
            functools.partial(close_backward, sweep == SWEEPS - 1),
            [block, block] + edges4,
            y, arr, recv, field, cols, uh, ul, w,
        )
        field, change, sends = out[0], out[1], out[2:]

    got = exchange(sends)

    def restrict(x_ref, a, b, c, d, cols_ref, fh_ref, fl_ref, rh_ref, rl_ref, lane_ref, res_ref, part_ref, near):
        cols = cols_ref[...]
        res = tangential(x_ref, (a, b, c, d), cols, (fh_ref, fl_ref), near, n, lx, ly)
        res_ref[...] = res
        proj = times(res, (rh_ref[...], rl_ref[...]))
        part = lax.broadcasted_iota(jnp.int32, (rows, width), 1) // cb
        proj = jnp.where(part.astype(F32) == cols[:, 19:20], proj, 0.0)
        hit = lax.broadcasted_iota(jnp.int32, (agg_rows, rows), 0).astype(F32)
        hit = jnp.where(hit == lane_ref[0:1, :], 1.0, 0.0).astype(BF16)
        hi, lo = halves(proj)
        part_ref[...] = nn(hit, hi) + nn(hit, lo)

    residual, partial = call(
        restrict,
        [block, ((agg_rows, width), F32)],
        change, *got, cols, fh, fl, rh, rl, agg_lane,
        scratch=[pltpu.VMEM((4, rows, width), F32)],
    )
    parts = lax.all_to_all(partial.reshape(owners, owned_rows, width), "ty", 0, 0, tiled=True)

    def solve_coarse(parts_ref, ch_ref, cl_ref, up_ref):
        sums = parts_ref[0]
        for k in range(1, owners):
            sums = sums + parts_ref[k]
        hi, lo = halves(sums)
        zero = jnp.zeros((8 - owned_rows, width), BF16)
        hi, lo = jnp.concatenate([hi, zero], 0), jnp.concatenate([lo, zero], 0)
        both = jnp.concatenate([hi, lo], 0)
        out = nt(both, ch_ref[...])
        out = out[:8] + out[8:] + nt(both, cl_ref[...])[:8]
        row = lax.broadcasted_iota(jnp.int32, (8, width), 0)
        acc = jnp.zeros((8, width), F32)
        for k in range(owned_rows):
            acc = acc + jnp.where(row == k, out[:, k * width : (k + 1) * width], 0.0)
        for k in range(owners):
            up_ref[k] = acc[:owned_rows]

    (copies,) = call(solve_coarse, [((owners, owned_rows, width), F32)], parts, ch, cl)
    update = lax.all_to_all(copies, "ty", 0, 0, tiled=True)

    def correct(up_ref, x_ref, cols_ref, rh_ref, rl_ref, out_ref):
        cols = cols_ref[...]
        hit = lax.broadcasted_iota(jnp.int32, (rows, agg_rows), 1).astype(F32)
        hit = jnp.where(hit == cols[:, 18:19], 1.0, 0.0).astype(BF16)
        hi, lo = halves(up_ref[...])
        picked = nn(hit, hi) + nn(hit, lo)
        part = lax.broadcasted_iota(jnp.int32, (rows, width), 1) // cb
        picked = jnp.where(part.astype(F32) == cols[:, 19:20], picked, 0.0)
        out_ref[...] = x_ref[...] + times(picked, (rh_ref[...], rl_ref[...]), nn)

    (corrected,) = call(correct, [block], update.reshape(agg_rows, width), field, cols, rh, rl)
    return corrected.reshape(right_side.shape), residual.reshape(right_side.shape)


def solution(mesh):
    in_specs = (
        P("line", "tx", "ty", None),
        P("line", "tx", "ty", None),
        P("line", "tx", "ty", None, None),
        P("line", "tx", "ty"),
        P("line", "tx", "ty"),
        P(),
        P(),
        P(),
        P(None, "line", "tx", "ty"),
        P(None, "line", "tx", "ty"),
        P("line", "tx", "ty"),
        P(),
        P("line", "tx", "ty", None, None),
    )
    out_specs = (P("line", "tx", "ty", None), P("line", "tx", "ty", None))
    return jax.shard_map(body, mesh=mesh, in_specs=in_specs, out_specs=out_specs, check_vma=False)
```
